8 devices in a mesh: mp: 2 (over z, y), dp: 4 (over x, core).
Axes of the slice: x: 2, y: 2, z: 1, core: 2. Of those that a mesh axis runs over, the one named last changes fastest.
Arguments:
- a_mat: bfloat16 [4096, 65536], P(('mp', 'dp'))
- b_mat: bfloat16 [65536, 4096], P(('mp', 'dp'))
Outputs:
- output: bfloat16 [4096, 4096], P(('mp', 'dp'))
All inputs are finite; a program needn't handle non-finite values.
Results may differ from the reference program's by a relative error of at most 0.001.
Values are sent between devices in bfloat16 or wider.
A program may use at most 1 GiB of HBM per device.

```python
import jax
import jax.numpy as jnp

M_DIM = 4096
N_DIM = 4096
TOKENS = 65536


def setup_inputs(seed: int = 0) -> dict:
    root_key = jax.random.key(seed)
    key_a, key_b = jax.random.split(root_key)
    a_mat = jax.random.normal(key_a, (M_DIM, TOKENS), jnp.float32)
    b_mat = jax.random.normal(key_b, (TOKENS, N_DIM), jnp.float32) * (TOKENS ** -0.5)
    return {"a_mat": a_mat.astype(jnp.bfloat16), "b_mat": b_mat.astype(jnp.bfloat16)}


def reference(a_mat, b_mat):
    return jnp.dot(a_mat, b_mat, preferred_element_type=jnp.float32).astype(jnp.bfloat16)
```

```python
import functools

import jax
import jax.numpy as jnp
from jax import lax
from jax.experimental import pallas as pl
from jax.experimental.pallas import tpu as pltpu
from jax.sharding import PartitionSpec as P

MESH = pl.DeviceIdType.MESH
N_TILES = 8
K_TILES = 4
WINDOW = 2
MIX_LAG = 2
END_LAG = 4
BUFS = END_LAG + 1
B_PIECES = 8


def _kernel(chunk, a_ref, b_ref, c_ref, b_par, a_in, leg1, leg2,
            a_v, b_v, acc, t1, t2, t3, c_v,
            bx_send, bx_recv, a_send, a_recv, l1_send, l1_recv, l2_send, l2_recv,
            a_sem, b_sem, t_sem, c_sem):
    rows = a_ref.shape[0]
    half_k, cols = b_ref.shape
    chip_k = 2 * half_k
    steps = rows // chunk
    nt = cols // N_TILES
    kt = chip_k // K_TILES
    own_tiles = K_TILES // 2

    mp = lax.axis_index("mp")
    dp = lax.axis_index("dp")
    core = lax.rem(dp, 2)
    xx = dp // 2
    flip_x = (1 - xx) * 2 + core
    flip_y = 1 - mp

    def coords(slot):
        is_x = 1 - slot // 2
        is_y = (slot + 1) // 2
        return mp + is_y * (1 - 2 * mp), xx + is_x * (1 - 2 * xx)

    barrier = pltpu.get_barrier_semaphore()
    for peer in ((mp, flip_x), (flip_y, dp), (flip_y, flip_x), (mp, xx * 2 + 1 - core)):
        pl.semaphore_signal(barrier, inc=1, device_id=peer, device_id_type=MESH)
    pl.semaphore_wait(barrier, 4)

    piece = half_k // B_PIECES

    def b_copy(j):
        span = pl.ds(j * piece, piece)
        return pltpu.make_async_remote_copy(
            src_ref=b_ref.at[span], dst_ref=b_par.at[span],
            send_sem=bx_send.at[j], recv_sem=bx_recv.at[j],
            device_id=(mp, xx * 2 + 1 - core), device_id_type=MESH)

    def a_copy(t, order):
        if order == 2:
            slot = 2
        else:
            slot = core if order == 0 else 1 - core
        to_mp, to_x = coords(slot)
        start = pl.multiple_of((to_mp * 2 + to_x) * chip_k, chip_k)
        span = pl.ds(pl.multiple_of(t * chunk, chunk), chunk)
        return pltpu.make_async_remote_copy(
            src_ref=a_ref.at[span, pl.ds(start, chip_k)],
            dst_ref=a_in.at[slot, span],
            send_sem=a_send.at[t, slot], recv_sem=a_recv.at[t, slot],
            device_id=(to_mp, to_x * 2 + core), device_id_type=MESH)

    def b_tile(n, k):
        src = b_ref if k < own_tiles else b_par
        return pltpu.make_async_copy(
            src.at[pl.ds((k % own_tiles) * kt, kt), pl.ds(pl.multiple_of(n * nt, nt), nt)],
            b_v.at[k], b_sem.at[k])

    for t in range(WINDOW):
        for order in range(3):
            a_copy(t, order).start()
    for j in range(B_PIECES):
        b_copy(j).start()
    for k in range(own_tiles):
        b_tile(0, k).start()
    for j in range(B_PIECES):
        b_copy(j).wait_recv()
    for k in range(own_tiles, K_TILES):
        b_tile(0, k).start()

    def leg1_copy(t):
        odd = lax.rem(t, 2)
        to_mp = mp + odd * (1 - 2 * mp)
        to_x = xx + (1 - odd) * (1 - 2 * xx)
        return pltpu.make_async_remote_copy(
            src_ref=acc.at[lax.rem(t, BUFS), pl.ds(pl.multiple_of((1 + odd) * chunk, chunk), 2 * chunk)],
            dst_ref=leg1.at[t], send_sem=l1_send.at[t], recv_sem=l1_recv.at[t],
            device_id=(to_mp, to_x * 2 + core), device_id_type=MESH)

    def leg2_copy(t):
        odd = lax.rem(t, 2)
        to_mp = mp + (1 - odd) * (1 - 2 * mp)
        to_x = xx + odd * (1 - 2 * xx)
        group = 3 - 2 * odd
        return pltpu.make_async_remote_copy(
            src_ref=acc.at[lax.rem(t, BUFS), pl.ds(pl.multiple_of(group * chunk, chunk), chunk)],
            dst_ref=leg2.at[t], send_sem=l2_send.at[t], recv_sem=l2_recv.at[t],
            device_id=(to_mp, to_x * 2 + core), device_id_type=MESH)

    def c_copy(t):
        slot = lax.rem(t, 2)
        return pltpu.make_async_copy(
            c_v.at[slot], c_ref.at[pl.ds(pl.multiple_of(t * chunk, chunk), chunk)], c_sem.at[slot])

    my_start = (mp * 2 + xx) * chip_k

    def product(t):
        for order in range(3):
            a_copy(t, order).wait_recv()

        span = pl.ds(pl.multiple_of(t * chunk, chunk), chunk)
        loads = []
        for h in range(2):
            off = (core + h - 2 * core * h) * half_k
            for g in range(4):
                if g == 0:
                    src = a_ref.at[span, pl.ds(pl.multiple_of(my_start + off, half_k), half_k)]
                else:
                    src = a_in.at[g - 1, span, pl.ds(pl.multiple_of(off, half_k), half_k)]
                loads.append(pltpu.make_async_copy(
                    src, a_v.at[pl.ds(g * chunk, chunk), pl.ds(h * half_k, half_k)],
                    a_sem.at[h * 4 + g]))
        for load in loads:
            load.start()

        for order in range(3):
            a_copy(t, order).wait_send()

        @pl.when(t + WINDOW < steps)
        def _():
            for order in range(3):
                a_copy(t + WINDOW, order).start()

        for load in loads:
            load.wait()

        buf = lax.rem(t, BUFS)

        def column(n, carry):
            place = pl.ds(pl.multiple_of(n * nt, nt), nt)
            for k in range(K_TILES):
                b_tile(n, k).wait()
                term = jnp.dot(a_v[:, k * kt:(k + 1) * kt], b_v[k],
                               preferred_element_type=jnp.float32)
                if k == 0:
                    acc[buf, :, place] = term
                else:
                    acc[buf, :, place] += term

                @pl.when(t * N_TILES + n < steps * N_TILES - 1)
                def _():
                    b_tile(lax.rem(n + 1, N_TILES), k).start()
            return carry

        lax.fori_loop(0, N_TILES, column, 0)
        leg1_copy(t).start()

    def forward(t):
        odd = lax.rem(t, 2)
        leg1_copy(t).wait_recv()
        load = pltpu.make_async_copy(
            leg1.at[t, pl.ds(pl.multiple_of((1 - odd) * chunk, chunk), chunk)], t1, t_sem.at[0])
        load.start()
        load.wait()
        group = 3 - 2 * odd
        place = pl.ds(pl.multiple_of(group * chunk, chunk), chunk)
        buf = lax.rem(t, BUFS)
        acc[buf, place] += t1[...]
        leg2_copy(t).start()

    def finish(t):
        odd = lax.rem(t, 2)
        leg2_copy(t).wait_recv()
        one = pltpu.make_async_copy(
            leg1.at[t, pl.ds(pl.multiple_of(odd * chunk, chunk), chunk)], t2, t_sem.at[1])
        two = pltpu.make_async_copy(leg2.at[t], t3, t_sem.at[2])
        one.start()
        two.start()

        @pl.when(t >= 2)
        def _():
            c_copy(t).wait()

        one.wait()
        two.wait()
        total = acc[lax.rem(t, BUFS), pl.ds(0, chunk)] + t2[...] + t3[...]
        c_v[lax.rem(t, 2)] = total.astype(c_v.dtype)
        leg1_copy(t).wait_send()
        leg2_copy(t).wait_send()
        c_copy(t).start()

    def step(s, carry):
        @pl.when(s < steps)
        def _():
            product(s)

        @pl.when((s >= MIX_LAG) & (s < steps + MIX_LAG))
        def _():
            forward(s - MIX_LAG)

        @pl.when(s >= END_LAG)
        def _():
            finish(s - END_LAG)
        return carry

    lax.fori_loop(0, steps + END_LAG, step, 0)
    for t in (steps - 2, steps - 1):
        c_copy(t).wait()
    for j in range(B_PIECES):
        b_copy(j).wait_send()


def _product(a_rows, b_rows, chunk):
    rows = a_rows.shape[0]
    half_k, cols = b_rows.shape
    steps = rows // chunk
    nt, kt = cols // N_TILES, 2 * half_k // K_TILES
    sem = pltpu.SemaphoreType.DMA
    hbm = pl.BlockSpec(memory_space=pl.ANY)
    outs = pl.pallas_call(
        functools.partial(_kernel, chunk),
        out_shape=(
            jax.ShapeDtypeStruct((rows, cols), jnp.bfloat16),
            jax.ShapeDtypeStruct((half_k, cols), jnp.bfloat16),
            jax.ShapeDtypeStruct((3, rows, 2 * half_k), jnp.bfloat16),
            jax.ShapeDtypeStruct((steps, 2 * chunk, cols), jnp.float32),
            jax.ShapeDtypeStruct((steps, chunk, cols), jnp.float32),
        ),
        in_specs=[hbm] * 2,
        out_specs=(hbm,) * 5,
        scratch_shapes=[
            pltpu.VMEM((4 * chunk, 2 * half_k), jnp.bfloat16),
            pltpu.VMEM((K_TILES, kt, nt), jnp.bfloat16),
            pltpu.VMEM((BUFS, 4 * chunk, cols), jnp.float32),
            pltpu.VMEM((chunk, cols), jnp.float32),
            pltpu.VMEM((chunk, cols), jnp.float32),
            pltpu.VMEM((chunk, cols), jnp.float32),
            pltpu.VMEM((2, chunk, cols), jnp.bfloat16),
            sem((B_PIECES,)), sem((B_PIECES,)),
            sem((steps, 3)), sem((steps, 3)),
            sem((steps,)), sem((steps,)), sem((steps,)), sem((steps,)),
            sem((8,)), sem((K_TILES,)), sem((3,)), sem((2,)),
        ],
        compiler_params=pltpu.CompilerParams(
            collective_id=0, has_side_effects=True, vmem_limit_bytes=60 << 20),
    )(a_rows, b_rows)
    return outs[0]


def solution(mesh):
    spec = P(("mp", "dp"), None)

    def local(a_rows, b_rows):
        return _product(a_rows, b_rows, min(32, a_rows.shape[0] // 4))

    return jax.shard_map(local, mesh=mesh, in_specs=(spec, spec), out_specs=spec, check_vma=False)
```

```python
import functools

import jax
import jax.numpy as jnp
from jax import lax
from jax.experimental import pallas as pl
from jax.experimental.pallas import tpu as pltpu
from jax.sharding import PartitionSpec as P

MESH = pl.DeviceIdType.MESH
N_TILES = 8
SLICES = 4
SLOTS = 4
AHEAD = 2
BUFS = 3
B_PIECES = 8


def _kernel(chunk, a_ref, b_ref, c_ref, b_par, a_in, leg1, leg2,
            a_v, b_v, acc, t1, t2, t3, c_v,
            bx_send, bx_recv, a_send, a_recv, l1_send, l1_recv, l2_send, l2_recv,
            a_sem, b_sem, t_sem, c_sem):
    rows = a_ref.shape[0]
    half_k, cols = b_ref.shape
    chip_k = 2 * half_k
    steps = rows // chunk
    half = chunk // 2
    nt = cols // N_TILES
    kt = chip_k // SLICES
    own_slices = SLICES // 2

    mp = lax.axis_index("mp")
    dp = lax.axis_index("dp")
    core = lax.rem(dp, 2)
    xx = dp // 2
    x_peer = (mp, (1 - xx) * 2 + core)
    y_peer = (1 - mp, dp)
    diagonal = (1 - mp, (1 - xx) * 2 + core)
    partner = (mp, xx * 2 + 1 - core)

    barrier = pltpu.get_barrier_semaphore()
    for peer in (x_peer, y_peer, diagonal, partner):
        pl.semaphore_signal(barrier, inc=1, device_id=peer, device_id_type=MESH)
    pl.semaphore_wait(barrier, 4)

    def chunk_rows(t):
        return pl.ds(pl.multiple_of(t * chunk, chunk), chunk)

    def slice_start(q):
        h = q // own_slices
        side = core + h - 2 * core * h
        return side * half_k + lax.rem(q, own_slices) * kt

    piece = half_k // B_PIECES

    def b_copy(j):
        span = pl.ds(j * piece, piece)
        return pltpu.make_async_remote_copy(
            src_ref=b_ref.at[span], dst_ref=b_par.at[span],
            send_sem=bx_send.at[j], recv_sem=bx_recv.at[j],
            device_id=partner, device_id_type=MESH)

    def a_copy(t, q, order):
        slot = 2 if order == 2 else (core if order == 0 else 1 - core)
        is_x = 1 - slot // 2
        is_y = (slot + 1) // 2
        to_mp = mp + is_y * (1 - 2 * mp)
        to_x = xx + is_x * (1 - 2 * xx)
        part = slice_start(q)
        start = pl.multiple_of((to_mp * 2 + to_x) * chip_k + part, kt)
        return pltpu.make_async_remote_copy(
            src_ref=a_ref.at[chunk_rows(t), pl.ds(start, kt)],
            dst_ref=a_in.at[slot, chunk_rows(t), pl.ds(pl.multiple_of(part, kt), kt)],
            send_sem=a_send.at[t, q, slot], recv_sem=a_recv.at[t, q, slot],
            device_id=(to_mp, to_x * 2 + core), device_id_type=MESH)

    def send_a(t):
        def body(q, carry):
            for order in range(3):
                a_copy(t, q, order).start()
            return carry
        lax.fori_loop(0, SLICES, body, 0)

    def sent_a(t):
        def body(q, carry):
            for order in range(3):
                a_copy(t, q, order).wait_send()
            return carry
        lax.fori_loop(0, SLICES, body, 0)

    def b_tile(src, q, n, slot):
        return pltpu.make_async_copy(
            src.at[pl.ds(pl.multiple_of(lax.rem(q, own_slices) * kt, kt), kt),
                   pl.ds(pl.multiple_of(n * nt, nt), nt)],
            b_v.at[slot], b_sem.at[slot])

    def load_tile(q, n, slot):
        @pl.when(q < own_slices)
        def _():
            b_tile(b_ref, q, n, slot).start()

        @pl.when(q >= own_slices)
        def _():
            b_tile(b_par, q, n, slot).start()

    for t in range(AHEAD):
        send_a(t)
    for j in range(B_PIECES):
        b_copy(j).start()
    for slot in range(SLOTS):
        b_tile(b_ref, 0, slot, slot).start()

    sources = [(0, half, 0), (1, half, 0), (2, half, 0), (0, half, half), (1, half, half), (2, half, half)]

    def a_loads(t, q):
        part = slice_start(q)
        mine = pl.multiple_of((mp * 2 + xx) * chip_k + part, kt)
        loads = [pltpu.make_async_copy(
            a_ref.at[chunk_rows(t), pl.ds(mine, kt)], a_v.at[q, pl.ds(0, chunk)], a_sem.at[6])]
        for i, (slot, size, off) in enumerate(sources):
            span = pl.ds(pl.multiple_of(t * chunk + off, half), half)
            loads.append(pltpu.make_async_copy(
                a_in.at[slot, span, pl.ds(pl.multiple_of(part, kt), kt)],
                a_v.at[q, pl.ds(chunk + i * half, half)], a_sem.at[i]))
        return loads

    def leg1_copies(t):
        buf = lax.rem(t, BUFS)
        return [pltpu.make_async_remote_copy(
            src_ref=acc.at[buf, pl.ds(start, chunk)], dst_ref=leg1.at[t, i],
            send_sem=l1_send.at[t, i], recv_sem=l1_recv.at[t, i],
            device_id=peer, device_id_type=MESH)
            for i, (start, peer) in enumerate(((chunk, x_peer), (chunk + 4 * half, y_peer)))]

    def leg2_copies(t):
        buf = lax.rem(t, BUFS)
        return [pltpu.make_async_remote_copy(
            src_ref=acc.at[buf, pl.ds(chunk + (2 + i) * half, half)],
            dst_ref=leg2.at[t, pl.ds(i * half, half)],
            send_sem=l2_send.at[t, i], recv_sem=l2_recv.at[t, i],
            device_id=peer, device_id_type=MESH)
            for i, peer in enumerate((y_peer, x_peer))]

    def c_copy(t):
        slot = lax.rem(t, 2)
        return pltpu.make_async_copy(c_v.at[slot], c_ref.at[chunk_rows(t)], c_sem.at[slot])

    def product(t):
        buf = lax.rem(t, BUFS)
        acc[buf] = jnp.zeros(acc.shape[1:], acc.dtype)

        def one_slice(q, carry):
            for order in range(3):
                a_copy(t, q, order).wait_recv()
            loads = a_loads(t, q)
            for load in loads:
                load.start()

            @pl.when((t == 0) & (q >= own_slices - 1) & (q < SLICES - 1))
            def _():
                def body(j, c):
                    b_copy(j).wait_recv()
                    return c
                per = B_PIECES // own_slices
                lax.fori_loop((q - own_slices + 1) * per, (q - own_slices + 2) * per, body, 0)

            for load in loads:
                load.wait()

            def columns(m, c):
                for slot in range(SLOTS):
                    n = m * SLOTS + slot
                    b_tile(b_ref, q, n, slot).wait()
                    acc[buf, :, pl.ds(pl.multiple_of(n * nt, nt), nt)] += jnp.dot(
                        a_v[q], b_v[slot], preferred_element_type=jnp.float32)
                    later = m + 1
                    wraps = later // (N_TILES // SLOTS)

                    @pl.when((t < steps - 1) | (q < SLICES - 1) | (wraps == 0))
                    def _():
                        load_tile(lax.rem(q + wraps, SLICES),
                                  (later - wraps * (N_TILES // SLOTS)) * SLOTS + slot, slot)
                return c

            lax.fori_loop(0, N_TILES // SLOTS, columns, 0)
            return carry

        lax.fori_loop(0, SLICES, one_slice, 0)

    def forward(t):
        copies = leg1_copies(t)
        for copy in copies:
            copy.wait_recv()
        loads = [pltpu.make_async_copy(
            leg1.at[t, i, pl.ds((1 - i) * half, half)], t1.at[pl.ds(i * half, half)], t_sem.at[i])
            for i in range(2)]
        for load in loads:
            load.start()
        for load in loads:
            load.wait()
        buf = lax.rem(t, BUFS)
        acc[buf, pl.ds(chunk + 2 * half, chunk)] += t1[...]
        for copy in leg2_copies(t):
            copy.start()

    def finish(t):
        loads = [pltpu.make_async_copy(
            leg1.at[t, i, pl.ds(i * half, half)], t2.at[pl.ds(i * half, half)], t_sem.at[2 + i])
            for i in range(2)]
        for load in loads:
            load.start()
        for copy in leg2_copies(t):
            copy.wait_recv()
        last = pltpu.make_async_copy(leg2.at[t], t3, t_sem.at[4])
        last.start()

        @pl.when(t >= 2)
        def _():
            c_copy(t).wait()

        for copy in leg1_copies(t) + leg2_copies(t):
            copy.wait_send()
        for load in loads:
            load.wait()
        last.wait()
        total = acc[lax.rem(t, BUFS), pl.ds(0, chunk)] + t2[...] + t3[...]
        c_v[lax.rem(t, 2)] = total.astype(c_v.dtype)
        c_copy(t).start()

    def step(s, carry):
        @pl.when(s < steps)
        def _():
            product(s)
            for copy in leg1_copies(s):
                copy.start()
            sent_a(s)

        @pl.when((s >= 1) & (s < steps + 1))
        def _():
            forward(s - 1)

        @pl.when(s + AHEAD < steps)
        def _():
            send_a(s + AHEAD)

        @pl.when(s >= 2)
        def _():
            finish(s - 2)
        return carry

    lax.fori_loop(0, steps + 2, step, 0)
    for t in (steps - 2, steps - 1):
        c_copy(t).wait()
    for j in range(B_PIECES):
        b_copy(j).wait_send()


def _product(a_rows, b_rows, chunk):
    rows = a_rows.shape[0]
    half_k, cols = b_rows.shape
    steps = rows // chunk
    nt, kt = cols // N_TILES, 2 * half_k // SLICES
    sem = pltpu.SemaphoreType.DMA
    hbm = pl.BlockSpec(memory_space=pl.ANY)
    outs = pl.pallas_call(
        functools.partial(_kernel, chunk),
        out_shape=(
            jax.ShapeDtypeStruct((rows, cols), jnp.bfloat16),
            jax.ShapeDtypeStruct((half_k, cols), jnp.bfloat16),
            jax.ShapeDtypeStruct((3, rows, 2 * half_k), jnp.bfloat16),
            jax.ShapeDtypeStruct((steps, 2, chunk, cols), jnp.float32),
            jax.ShapeDtypeStruct((steps, chunk, cols), jnp.float32),
        ),
        in_specs=[hbm] * 2,
        out_specs=(hbm,) * 5,
        scratch_shapes=[
            pltpu.VMEM((SLICES, 4 * chunk, kt), jnp.bfloat16),
            pltpu.VMEM((SLOTS, kt, nt), jnp.bfloat16),
            pltpu.VMEM((BUFS, 4 * chunk, cols), jnp.float32),
            pltpu.VMEM((chunk, cols), jnp.float32),
            pltpu.VMEM((chunk, cols), jnp.float32),
            pltpu.VMEM((chunk, cols), jnp.float32),
            pltpu.VMEM((2, chunk, cols), jnp.bfloat16),
            sem((B_PIECES,)), sem((B_PIECES,)),
            sem((steps, SLICES, 3)), sem((steps, SLICES, 3)),
            sem((steps, 2)), sem((steps, 2)), sem((steps, 2)), sem((steps, 2)),
            sem((7,)), sem((SLOTS,)), sem((5,)), sem((2,)),
        ],
        compiler_params=pltpu.CompilerParams(
            collective_id=0, has_side_effects=True, vmem_limit_bytes=60 << 20),
    )(a_rows, b_rows)
    return outs[0]


def solution(mesh):
    spec = P(("mp", "dp"), None)

    def local(a_rows, b_rows):
        return _product(a_rows, b_rows, min(64, a_rows.shape[0] // 4))

    return jax.shard_map(local, mesh=mesh, in_specs=(spec, spec), out_specs=spec, check_vma=False)
```

```python
import functools

import jax
import jax.numpy as jnp
from jax import lax
from jax.experimental import pallas as pl
from jax.experimental.pallas import tpu as pltpu
from jax.sharding import PartitionSpec as P

MESH = pl.DeviceIdType.MESH
N_TILES = 8
SLICES = 4
SLOTS = 4
AHEAD = 2
BUFS = 3
B_PIECES = 8


def _kernel(chunk, a_ref, b_ref, c_ref, b_par, a_in, leg1,
            a_v, b_v, acc, t1, t2, leg2,
            bx_send, bx_recv, a_send, a_recv, l1_send, l1_recv, l2_send, l2_recv,
            a_sem, b_sem, t_sem):
    rows = a_ref.shape[0]
    half_k, cols = b_ref.shape
    chip_k = 2 * half_k
    steps = rows // chunk
    half = chunk // 2
    nt = cols // N_TILES
    kt = chip_k // SLICES
    own_slices = SLICES // 2

    mp = lax.axis_index("mp")
    dp = lax.axis_index("dp")
    core = lax.rem(dp, 2)
    xx = dp // 2
    x_peer = (mp, (1 - xx) * 2 + core)
    y_peer = (1 - mp, dp)
    diagonal = (1 - mp, (1 - xx) * 2 + core)
    partner = (mp, xx * 2 + 1 - core)

    barrier = pltpu.get_barrier_semaphore()
    for peer in (x_peer, y_peer, diagonal, partner):
        pl.semaphore_signal(barrier, inc=1, device_id=peer, device_id_type=MESH)
    pl.semaphore_wait(barrier, 4)

    def chunk_rows(t):
        return pl.ds(pl.multiple_of(t * chunk, chunk), chunk)

    def slice_start(q):
        h = q // own_slices
        side = core + h - 2 * core * h
        return side * half_k + lax.rem(q, own_slices) * kt

    piece = half_k // B_PIECES

    def b_copy(j):
        span = pl.ds(j * piece, piece)
        return pltpu.make_async_remote_copy(
            src_ref=b_ref.at[span], dst_ref=b_par.at[span],
            send_sem=bx_send.at[j], recv_sem=bx_recv.at[j],
            device_id=partner, device_id_type=MESH)

    def a_copy(t, q, order):
        slot = 2 if order == 2 else (core if order == 0 else 1 - core)
        is_x = 1 - slot // 2
        is_y = (slot + 1) // 2
        to_mp = mp + is_y * (1 - 2 * mp)
        to_x = xx + is_x * (1 - 2 * xx)
        part = slice_start(q)
        start = pl.multiple_of((to_mp * 2 + to_x) * chip_k + part, kt)
        return pltpu.make_async_remote_copy(
            src_ref=a_ref.at[chunk_rows(t), pl.ds(start, kt)],
            dst_ref=a_in.at[slot, chunk_rows(t), pl.ds(pl.multiple_of(part, kt), kt)],
            send_sem=a_send.at[t, q, slot], recv_sem=a_recv.at[t, q, slot],
            device_id=(to_mp, to_x * 2 + core), device_id_type=MESH)

    def send_a(t):
        def body(q, carry):
            for order in range(3):
                a_copy(t, q, order).start()
            return carry
        lax.fori_loop(0, SLICES, body, 0)

    def sent_a(t):
        def body(q, carry):
            for order in range(3):
                a_copy(t, q, order).wait_send()
            return carry
        lax.fori_loop(0, SLICES, body, 0)

    def b_tile(src, q, n, slot):
        return pltpu.make_async_copy(
            src.at[pl.ds(pl.multiple_of(lax.rem(q, own_slices) * kt, kt), kt),
                   pl.ds(pl.multiple_of(n * nt, nt), nt)],
            b_v.at[slot], b_sem.at[slot])

    def load_tile(q, n, slot):
        @pl.when(q < own_slices)
        def _():
            b_tile(b_ref, q, n, slot).start()

        @pl.when(q >= own_slices)
        def _():
            b_tile(b_par, q, n, slot).start()

    for t in range(AHEAD):
        send_a(t)
    for j in range(B_PIECES):
        b_copy(j).start()
    for slot in range(SLOTS):
        b_tile(b_ref, 0, slot, slot).start()

    sources = [(0, half, 0), (1, half, 0), (2, half, 0), (0, half, half), (1, half, half), (2, half, half)]

    def a_loads(t, q):
        part = slice_start(q)
        mine = pl.multiple_of((mp * 2 + xx) * chip_k + part, kt)
        loads = [pltpu.make_async_copy(
            a_ref.at[chunk_rows(t), pl.ds(mine, kt)], a_v.at[q, pl.ds(0, chunk)], a_sem.at[6])]
        for i, (slot, size, off) in enumerate(sources):
            span = pl.ds(pl.multiple_of(t * chunk + off, half), half)
            loads.append(pltpu.make_async_copy(
                a_in.at[slot, span, pl.ds(pl.multiple_of(part, kt), kt)],
                a_v.at[q, pl.ds(chunk + i * half, half)], a_sem.at[i]))
        return loads

    def leg1_copies(t):
        buf = lax.rem(t, BUFS)
        return [pltpu.make_async_remote_copy(
            src_ref=acc.at[buf, pl.ds(start, chunk)], dst_ref=leg1.at[t, i],
            send_sem=l1_send.at[t, i], recv_sem=l1_recv.at[t, i],
            device_id=peer, device_id_type=MESH)
            for i, (start, peer) in enumerate(((chunk, x_peer), (chunk + 4 * half, y_peer)))]

    def leg2_copies(t):
        buf = lax.rem(t, BUFS)
        return [pltpu.make_async_remote_copy(
            src_ref=acc.at[buf, pl.ds(chunk + (2 + i) * half, half)],
            dst_ref=leg2.at[t, pl.ds(i * half, half)],
            send_sem=l2_send.at[t, i], recv_sem=l2_recv.at[t, i],
            device_id=peer, device_id_type=MESH)
            for i, peer in enumerate((y_peer, x_peer))]

    def product(t):
        buf = lax.rem(t, BUFS)
        acc[buf] = jnp.zeros(acc.shape[1:], acc.dtype)

        def one_slice(q, carry):
            for order in range(3):
                a_copy(t, q, order).wait_recv()
            loads = a_loads(t, q)
            for load in loads:
                load.start()

            @pl.when((t == 0) & (q >= own_slices - 1) & (q < SLICES - 1))
            def _():
                def body(j, c):
                    b_copy(j).wait_recv()
                    return c
                per = B_PIECES // own_slices
                lax.fori_loop((q - own_slices + 1) * per, (q - own_slices + 2) * per, body, 0)

            for load in loads:
                load.wait()

            def columns(m, c):
                for slot in range(SLOTS):
                    n = m * SLOTS + slot
                    b_tile(b_ref, q, n, slot).wait()
                    acc[buf, :, pl.ds(pl.multiple_of(n * nt, nt), nt)] += jnp.dot(
                        a_v[q], b_v[slot], preferred_element_type=jnp.float32)
                    later = m + 1
                    wraps = later // (N_TILES // SLOTS)

                    @pl.when((t < steps - 1) | (q < SLICES - 1) | (wraps == 0))
                    def _():
                        load_tile(lax.rem(q + wraps, SLICES),
                                  (later - wraps * (N_TILES // SLOTS)) * SLOTS + slot, slot)
                return c

            lax.fori_loop(0, N_TILES // SLOTS, columns, 0)
            return carry

        lax.fori_loop(0, SLICES, one_slice, 0)

    def forward(t):
        copies = leg1_copies(t)
        for copy in copies:
            copy.wait_recv()
        loads = [pltpu.make_async_copy(
            leg1.at[t, i, pl.ds((1 - i) * half, half)], t1.at[pl.ds(i * half, half)], t_sem.at[i])
            for i in range(2)]
        for load in loads:
            load.start()
        for load in loads:
            load.wait()
        buf = lax.rem(t, BUFS)
        acc[buf, pl.ds(chunk + 2 * half, chunk)] += t1[...]
        for copy in leg2_copies(t):
            copy.start()

    def finish(t):
        loads = [pltpu.make_async_copy(
            leg1.at[t, i, pl.ds(i * half, half)], t2.at[pl.ds(i * half, half)], t_sem.at[2 + i])
            for i in range(2)]
        for load in loads:
            load.start()
        for load in loads:
            load.wait()
        for copy in leg2_copies(t):
            copy.wait_recv()
        total = acc[lax.rem(t, BUFS), pl.ds(0, chunk)] + t2[...] + leg2[t]
        c_ref[chunk_rows(t)] = total.astype(c_ref.dtype)
        for copy in leg1_copies(t) + leg2_copies(t):
            copy.wait_send()

    def step(s, carry):
        @pl.when(s < steps)
        def _():
            product(s)
            for copy in leg1_copies(s):
                copy.start()
            sent_a(s)

        @pl.when((s >= 1) & (s < steps + 1))
        def _():
            forward(s - 1)

        @pl.when(s + AHEAD < steps)
        def _():
            send_a(s + AHEAD)

        @pl.when(s >= 2)
        def _():
            finish(s - 2)
        return carry

    lax.fori_loop(0, steps + 2, step, 0)
    for j in range(B_PIECES):
        b_copy(j).wait_send()


def _product(a_rows, b_rows, chunk):
    rows = a_rows.shape[0]
    half_k, cols = b_rows.shape
    steps = rows // chunk
    nt, kt = cols // N_TILES, 2 * half_k // SLICES
    sem = pltpu.SemaphoreType.DMA
    hbm = pl.BlockSpec(memory_space=pl.ANY)
    outs = pl.pallas_call(
        functools.partial(_kernel, chunk),
        out_shape=(
            pltpu.VMEM((rows, cols), jnp.bfloat16),
            jax.ShapeDtypeStruct((half_k, cols), jnp.bfloat16),
            jax.ShapeDtypeStruct((3, rows, 2 * half_k), jnp.bfloat16),
            jax.ShapeDtypeStruct((steps, 2, chunk, cols), jnp.float32),
        ),
        in_specs=[hbm] * 2,
        out_specs=(pl.BlockSpec(memory_space=pltpu.VMEM),) + (hbm,) * 3,
        scratch_shapes=[
            pltpu.VMEM((SLICES, 4 * chunk, kt), jnp.bfloat16),
            pltpu.VMEM((SLOTS, kt, nt), jnp.bfloat16),
            pltpu.VMEM((BUFS, 4 * chunk, cols), jnp.float32),
            pltpu.VMEM((chunk, cols), jnp.float32),
            pltpu.VMEM((chunk, cols), jnp.float32),
            pltpu.VMEM((steps, chunk, cols), jnp.float32),
            sem((B_PIECES,)), sem((B_PIECES,)),
            sem((steps, SLICES, 3)), sem((steps, SLICES, 3)),
            sem((steps, 2)), sem((steps, 2)), sem((steps, 2)), sem((steps, 2)),
            sem((7,)), sem((SLOTS,)), sem((4,)),
        ],
        compiler_params=pltpu.CompilerParams(
            collective_id=0, has_side_effects=True, vmem_limit_bytes=56 << 20),
    )(a_rows, b_rows)
    return outs[0]


def solution(mesh):
    spec = P(("mp", "dp"), None)

    def local(a_rows, b_rows):
        return _product(a_rows, b_rows, min(64, a_rows.shape[0] // 4))

    return jax.shard_map(local, mesh=mesh, in_specs=(spec, spec), out_specs=spec, check_vma=False)
```

```python
import functools

import jax
import jax.numpy as jnp
from jax import lax
from jax.experimental import pallas as pl
from jax.experimental.pallas import tpu as pltpu
from jax.sharding import PartitionSpec as P

MESH = pl.DeviceIdType.MESH
N_TILES = 8
SLICES = 4
SLOTS = 4
AHEAD = 2
BUFS = 3
B_PIECES = 8


def _kernel(chunk, a_ref, b_ref, c_ref, b_par, a_in, leg1,
            a_v, b_v, acc, t1, t2, leg2,
            bx_send, bx_recv, a_send, a_recv, l1_send, l1_recv, l2_send, l2_recv,
            a_sem, b_sem, t_sem, diag_sem):
    rows = a_ref.shape[0]
    half_k, cols = b_ref.shape
    chip_k = 2 * half_k
    steps = rows // chunk
    half = chunk // 2
    nt = cols // N_TILES
    kt = chip_k // SLICES
    own_slices = SLICES // 2

    mp = lax.axis_index("mp")
    dp = lax.axis_index("dp")
    core = lax.rem(dp, 2)
    xx = dp // 2
    x_peer = (mp, (1 - xx) * 2 + core)
    y_peer = (1 - mp, dp)
    partner = (mp, xx * 2 + 1 - core)

    barrier = pltpu.get_barrier_semaphore()
    for peer in (x_peer, y_peer, partner):
        pl.semaphore_signal(barrier, inc=1, device_id=peer, device_id_type=MESH)
    pl.semaphore_wait(barrier, 3)

    def chunk_rows(t):
        return pl.ds(pl.multiple_of(t * chunk, chunk), chunk)

    def slice_start(q):
        h = q // own_slices
        side = core + h - 2 * core * h
        return side * half_k + lax.rem(q, own_slices) * kt

    piece = half_k // B_PIECES

    def b_copy(j):
        span = pl.ds(j * piece, piece)
        return pltpu.make_async_remote_copy(
            src_ref=b_ref.at[span], dst_ref=b_par.at[span],
            send_sem=bx_send.at[j], recv_sem=bx_recv.at[j],
            device_id=partner, device_id_type=MESH)

    def a_copy(t, q, order):
        slot = 2 if order == 2 else (core if order == 0 else 1 - core)
        return a_copy_to(t, q, slot)

    def a_copy_to(t, q, slot):
        is_x = 1 - slot // 2
        is_y = (slot + 1) // 2
        to_mp = mp + is_y * (1 - 2 * mp)
        to_x = xx + is_x * (1 - 2 * xx)
        part = slice_start(q)
        start = pl.multiple_of((to_mp * 2 + to_x) * chip_k + part, kt)
        return pltpu.make_async_remote_copy(
            src_ref=a_ref.at[chunk_rows(t), pl.ds(start, kt)],
            dst_ref=a_in.at[slot, chunk_rows(t), pl.ds(pl.multiple_of(part, kt), kt)],
            send_sem=a_send.at[t, q, slot], recv_sem=a_recv.at[t, q, slot],
            device_id=(to_mp, to_x * 2 + core), device_id_type=MESH)

    def send_a(t, first=0):
        def body(q, carry):
            for order in range(3):
                a_copy(t, q, order).start()
            return carry
        lax.fori_loop(first, SLICES, body, 0)

    def sent_a(t):
        def body(q, carry):
            for order in range(3):
                a_copy(t, q, order).wait_send()
            return carry
        lax.fori_loop(0, SLICES, body, 0)

    def b_tile(src, q, n, slot):
        return pltpu.make_async_copy(
            src.at[pl.ds(pl.multiple_of(lax.rem(q, own_slices) * kt, kt), kt),
                   pl.ds(pl.multiple_of(n * nt, nt), nt)],
            b_v.at[slot], b_sem.at[slot])

    def load_tile(q, n, slot):
        @pl.when(q < own_slices)
        def _():
            b_tile(b_ref, q, n, slot).start()

        @pl.when(q >= own_slices)
        def _():
            b_tile(b_par, q, n, slot).start()

    a_copy_to(0, 0, 0).start()
    a_copy_to(0, 0, 2).start()
    pl.semaphore_signal(diag_sem, inc=1, device_id=y_peer, device_id_type=MESH)
    pl.semaphore_wait(diag_sem, 1)
    a_copy_to(0, 0, 1).start()
    send_a(0, 1)
    for t in range(1, AHEAD):
        send_a(t)
    for j in range(B_PIECES):
        b_copy(j).start()
    for slot in range(SLOTS):
        b_tile(b_ref, 0, slot, slot).start()

    sources = [(0, half, 0), (1, half, 0), (2, half, 0), (0, half, half), (1, half, half), (2, half, half)]

    def a_loads(t, q):
        part = slice_start(q)
        mine = pl.multiple_of((mp * 2 + xx) * chip_k + part, kt)
        loads = [pltpu.make_async_copy(
            a_ref.at[chunk_rows(t), pl.ds(mine, kt)], a_v.at[q, pl.ds(0, chunk)], a_sem.at[6])]
        for i, (slot, size, off) in enumerate(sources):
            span = pl.ds(pl.multiple_of(t * chunk + off, half), half)
            loads.append(pltpu.make_async_copy(
                a_in.at[slot, span, pl.ds(pl.multiple_of(part, kt), kt)],
                a_v.at[q, pl.ds(chunk + i * half, half)], a_sem.at[i]))
        return loads

    def leg1_copies(t):
        buf = lax.rem(t, BUFS)
        return [pltpu.make_async_remote_copy(
            src_ref=acc.at[buf, pl.ds(start, chunk)], dst_ref=leg1.at[t, i],
            send_sem=l1_send.at[t, i], recv_sem=l1_recv.at[t, i],
            device_id=peer, device_id_type=MESH)
            for i, (start, peer) in enumerate(((chunk, x_peer), (chunk + 4 * half, y_peer)))]

    def leg2_copies(t):
        buf = lax.rem(t, BUFS)
        return [pltpu.make_async_remote_copy(
            src_ref=acc.at[buf, pl.ds(chunk + (2 + i) * half, half)],
            dst_ref=leg2.at[t, pl.ds(i * half, half)],
            send_sem=l2_send.at[t, i], recv_sem=l2_recv.at[t, i],
            device_id=peer, device_id_type=MESH)
            for i, peer in enumerate((y_peer, x_peer))]

    def product(t):
        buf = lax.rem(t, BUFS)
        acc[buf] = jnp.zeros(acc.shape[1:], acc.dtype)

        def one_slice(q, carry):
            for order in range(3):
                a_copy(t, q, order).wait_recv()
            loads = a_loads(t, q)
            for load in loads:
                load.start()

            @pl.when((t == 0) & (q >= own_slices - 1) & (q < SLICES - 1))
            def _():
                def body(j, c):
                    b_copy(j).wait_recv()
                    return c
                per = B_PIECES // own_slices
                lax.fori_loop((q - own_slices + 1) * per, (q - own_slices + 2) * per, body, 0)

            for load in loads:
                load.wait()

            def columns(m, c):
                for slot in range(SLOTS):
                    n = m * SLOTS + slot
                    b_tile(b_ref, q, n, slot).wait()
                    acc[buf, :, pl.ds(pl.multiple_of(n * nt, nt), nt)] += jnp.dot(
                        a_v[q], b_v[slot], preferred_element_type=jnp.float32)
                    later = m + 1
                    wraps = later // (N_TILES // SLOTS)

                    @pl.when((t < steps - 1) | (q < SLICES - 1) | (wraps == 0))
                    def _():
                        load_tile(lax.rem(q + wraps, SLICES),
                                  (later - wraps * (N_TILES // SLOTS)) * SLOTS + slot, slot)
                return c

            lax.fori_loop(0, N_TILES // SLOTS, columns, 0)
            return carry

        lax.fori_loop(0, SLICES, one_slice, 0)

    def forward(t):
        copies = leg1_copies(t)
        for copy in copies:
            copy.wait_recv()
        loads = [pltpu.make_async_copy(
            leg1.at[t, i, pl.ds((1 - i) * half, half)], t1.at[pl.ds(i * half, half)], t_sem.at[i])
            for i in range(2)]
        for load in loads:
            load.start()
        for load in loads:
            load.wait()
        buf = lax.rem(t, BUFS)
        acc[buf, pl.ds(chunk + 2 * half, chunk)] += t1[...]
        for copy in leg2_copies(t):
            copy.start()

    def finish(t):
        loads = [pltpu.make_async_copy(
            leg1.at[t, i, pl.ds(i * half, half)], t2.at[pl.ds(i * half, half)], t_sem.at[2 + i])
            for i in range(2)]
        for load in loads:
            load.start()
        for load in loads:
            load.wait()
        for copy in leg2_copies(t):
            copy.wait_recv()
        total = acc[lax.rem(t, BUFS), pl.ds(0, chunk)] + t2[...] + leg2[t]
        c_ref[chunk_rows(t)] = total.astype(c_ref.dtype)
        for copy in leg1_copies(t) + leg2_copies(t):
            copy.wait_send()

    def step(s, carry):
        @pl.when(s < steps)
        def _():
            product(s)
            for copy in leg1_copies(s):
                copy.start()
            sent_a(s)

        @pl.when((s >= 1) & (s < steps + 1))
        def _():
            forward(s - 1)

        @pl.when(s + AHEAD < steps)
        def _():
            send_a(s + AHEAD)

        @pl.when(s >= 2)
        def _():
            finish(s - 2)
        return carry

    lax.fori_loop(0, steps + 2, step, 0)
    for j in range(B_PIECES):
        b_copy(j).wait_send()


def _product(a_rows, b_rows, chunk):
    rows = a_rows.shape[0]
    half_k, cols = b_rows.shape
    steps = rows // chunk
    nt, kt = cols // N_TILES, 2 * half_k // SLICES
    sem = pltpu.SemaphoreType.DMA
    hbm = pl.BlockSpec(memory_space=pl.ANY)
    outs = pl.pallas_call(
        functools.partial(_kernel, chunk),
        out_shape=(
            pltpu.VMEM((rows, cols), jnp.bfloat16),
            jax.ShapeDtypeStruct((half_k, cols), jnp.bfloat16),
            jax.ShapeDtypeStruct((3, rows, 2 * half_k), jnp.bfloat16),
            jax.ShapeDtypeStruct((steps, 2, chunk, cols), jnp.float32),
        ),
        in_specs=[hbm] * 2,
        out_specs=(pl.BlockSpec(memory_space=pltpu.VMEM),) + (hbm,) * 3,
        scratch_shapes=[
            pltpu.VMEM((SLICES, 4 * chunk, kt), jnp.bfloat16),
            pltpu.VMEM((SLOTS, kt, nt), jnp.bfloat16),
            pltpu.VMEM((BUFS, 4 * chunk, cols), jnp.float32),
            pltpu.VMEM((chunk, cols), jnp.float32),
            pltpu.VMEM((chunk, cols), jnp.float32),
            pltpu.VMEM((steps, chunk, cols), jnp.float32),
            sem((B_PIECES,)), sem((B_PIECES,)),
            sem((steps, SLICES, 3)), sem((steps, SLICES, 3)),
            sem((steps, 2)), sem((steps, 2)), sem((steps, 2)), sem((steps, 2)),
            sem((7,)), sem((SLOTS,)), sem((4,)), pltpu.SemaphoreType.REGULAR,
        ],
        compiler_params=pltpu.CompilerParams(
            collective_id=0, has_side_effects=True, vmem_limit_bytes=56 << 20),
    )(a_rows, b_rows)
    return outs[0]


def solution(mesh):
    spec = P(("mp", "dp"), None)

    def local(a_rows, b_rows):
        return _product(a_rows, b_rows, min(64, a_rows.shape[0] // 4))

    return jax.shard_map(local, mesh=mesh, in_specs=(spec, spec), out_specs=spec, check_vma=False)
```

```python
import functools

import jax
import jax.numpy as jnp
from jax import lax
from jax.experimental import pallas as pl
from jax.experimental.pallas import tpu as pltpu
from jax.sharding import PartitionSpec as P

MESH = pl.DeviceIdType.MESH
N_TILES = 8
SLICES = 4
SLOTS = 4
AHEAD = 2
BUFS = 3
RING = 4
B_PIECES = 8


def _kernel(chunk, a_ref, b_ref, c_ref, b_par, a_in,
            a_v, b_v, acc, leg1, leg2,
            bx_send, bx_recv, a_send, a_recv, l1_send, l1_recv, l2_send, l2_recv,
            a_sem, b_sem):
    rows = a_ref.shape[0]
    half_k, cols = b_ref.shape
    chip_k = 2 * half_k
    steps = rows // chunk
    half = chunk // 2
    nt = cols // N_TILES
    kt = chip_k // SLICES
    own_slices = SLICES // 2

    mp = lax.axis_index("mp")
    dp = lax.axis_index("dp")
    core = lax.rem(dp, 2)
    xx = dp // 2
    x_peer = (mp, (1 - xx) * 2 + core)
    y_peer = (1 - mp, dp)
    diagonal = (1 - mp, (1 - xx) * 2 + core)
    partner = (mp, xx * 2 + 1 - core)

    barrier = pltpu.get_barrier_semaphore()
    for peer in (x_peer, y_peer, diagonal, partner):
        pl.semaphore_signal(barrier, inc=1, device_id=peer, device_id_type=MESH)
    pl.semaphore_wait(barrier, 4)

    def chunk_rows(t):
        return pl.ds(pl.multiple_of(t * chunk, chunk), chunk)

    def slice_start(q):
        h = q // own_slices
        side = core + h - 2 * core * h
        return side * half_k + lax.rem(q, own_slices) * kt

    piece = half_k // B_PIECES

    def b_copy(j):
        span = pl.ds(j * piece, piece)
        return pltpu.make_async_remote_copy(
            src_ref=b_ref.at[span], dst_ref=b_par.at[span],
            send_sem=bx_send.at[j], recv_sem=bx_recv.at[j],
            device_id=partner, device_id_type=MESH)

    def a_copy(t, q, order):
        slot = 2 if order == 2 else (core if order == 0 else 1 - core)
        is_x = 1 - slot // 2
        is_y = (slot + 1) // 2
        to_mp = mp + is_y * (1 - 2 * mp)
        to_x = xx + is_x * (1 - 2 * xx)
        part = slice_start(q)
        start = pl.multiple_of((to_mp * 2 + to_x) * chip_k + part, kt)
        return pltpu.make_async_remote_copy(
            src_ref=a_ref.at[chunk_rows(t), pl.ds(start, kt)],
            dst_ref=a_in.at[slot, chunk_rows(t), pl.ds(pl.multiple_of(part, kt), kt)],
            send_sem=a_send.at[t, q, slot], recv_sem=a_recv.at[t, q, slot],
            device_id=(to_mp, to_x * 2 + core), device_id_type=MESH)

    def send_a(t):
        def body(q, carry):
            for order in range(3):
                a_copy(t, q, order).start()
            return carry
        lax.fori_loop(0, SLICES, body, 0)

    def sent_a(t):
        def body(q, carry):
            for order in range(3):
                a_copy(t, q, order).wait_send()
            return carry
        lax.fori_loop(0, SLICES, body, 0)

    def b_tile(src, q, n, slot):
        return pltpu.make_async_copy(
            src.at[pl.ds(pl.multiple_of(lax.rem(q, own_slices) * kt, kt), kt),
                   pl.ds(pl.multiple_of(n * nt, nt), nt)],
            b_v.at[slot], b_sem.at[slot])

    def load_tile(q, n, slot):
        @pl.when(q < own_slices)
        def _():
            b_tile(b_ref, q, n, slot).start()

        @pl.when(q >= own_slices)
        def _():
            b_tile(b_par, q, n, slot).start()

    for t in range(AHEAD):
        send_a(t)
    for j in range(B_PIECES):
        b_copy(j).start()
    for slot in range(SLOTS):
        b_tile(b_ref, 0, slot, slot).start()

    sources = [(0, half, 0), (1, half, 0), (2, half, 0), (0, half, half), (1, half, half), (2, half, half)]

    def a_loads(t, q):
        part = slice_start(q)
        mine = pl.multiple_of((mp * 2 + xx) * chip_k + part, kt)
        loads = [pltpu.make_async_copy(
            a_ref.at[chunk_rows(t), pl.ds(mine, kt)], a_v.at[q, pl.ds(0, chunk)],
            a_sem.at[lax.rem(q, 2), 6])]
        for i, (slot, size, off) in enumerate(sources):
            span = pl.ds(pl.multiple_of(t * chunk + off, half), half)
            loads.append(pltpu.make_async_copy(
                a_in.at[slot, span, pl.ds(pl.multiple_of(part, kt), kt)],
                a_v.at[q, pl.ds(chunk + i * half, half)], a_sem.at[lax.rem(q, 2), i]))
        return loads

    def leg1_copies(t):
        buf = lax.rem(t, BUFS)
        return [pltpu.make_async_remote_copy(
            src_ref=acc.at[buf, pl.ds(start, chunk)], dst_ref=leg1.at[lax.rem(t, RING), i],
            send_sem=l1_send.at[t, i], recv_sem=l1_recv.at[t, i],
            device_id=peer, device_id_type=MESH)
            for i, (start, peer) in enumerate(((chunk, x_peer), (chunk + 4 * half, y_peer)))]

    def leg2_copies(t):
        buf = lax.rem(t, BUFS)
        return [pltpu.make_async_remote_copy(
            src_ref=acc.at[buf, pl.ds(chunk + (2 + i) * half, half)],
            dst_ref=leg2.at[lax.rem(t, RING), pl.ds(i * half, half)],
            send_sem=l2_send.at[t, i], recv_sem=l2_recv.at[t, i],
            device_id=peer, device_id_type=MESH)
            for i, peer in enumerate((y_peer, x_peer))]

    def product(t):
        buf = lax.rem(t, BUFS)
        acc[buf] = jnp.zeros(acc.shape[1:], acc.dtype)

        def fetch(q):
            for order in range(3):
                a_copy(t, q, order).wait_recv()
            for load in a_loads(t, q):
                load.start()

        fetch(0)

        def one_slice(q, carry):
            @pl.when(q < SLICES - 1)
            def _():
                fetch(q + 1)

            @pl.when((t == 0) & (q >= own_slices - 1) & (q < SLICES - 1))
            def _():
                def body(j, c):
                    b_copy(j).wait_recv()
                    return c
                per = B_PIECES // own_slices
                lax.fori_loop((q - own_slices + 1) * per, (q - own_slices + 2) * per, body, 0)

            for load in a_loads(t, q):
                load.wait()

            def columns(m, c):
                for slot in range(SLOTS):
                    n = m * SLOTS + slot
                    b_tile(b_ref, q, n, slot).wait()
                    acc[buf, :, pl.ds(pl.multiple_of(n * nt, nt), nt)] += jnp.dot(
                        a_v[q], b_v[slot], preferred_element_type=jnp.float32)
                    later = m + 1
                    wraps = later // (N_TILES // SLOTS)

                    @pl.when((t < steps - 1) | (q < SLICES - 1) | (wraps == 0))
                    def _():
                        load_tile(lax.rem(q + wraps, SLICES),
                                  (later - wraps * (N_TILES // SLOTS)) * SLOTS + slot, slot)
                return c

            lax.fori_loop(0, N_TILES // SLOTS, columns, 0)
            return carry

        lax.fori_loop(0, SLICES, one_slice, 0)

    def forward(t):
        for copy in leg1_copies(t):
            copy.wait_recv()
        buf, slot = lax.rem(t, BUFS), lax.rem(t, RING)
        for i in range(2):
            acc[buf, pl.ds(chunk + (2 + i) * half, half)] += leg1[slot, i, pl.ds((1 - i) * half, half)]
        for copy in leg2_copies(t):
            copy.start()

    def finish(t):
        for copy in leg2_copies(t):
            copy.wait_recv()
        buf, slot = lax.rem(t, BUFS), lax.rem(t, RING)
        for i in range(2):
            part = pl.ds(i * half, half)
            total = acc[buf, part] + leg1[slot, i, part] + leg2[slot, part]
            c_ref[pl.ds(pl.multiple_of(t * chunk + i * half, half), half)] = total.astype(c_ref.dtype)
        for copy in leg1_copies(t) + leg2_copies(t):
            copy.wait_send()

    def step(s, carry):
        @pl.when(s < steps)
        def _():
            product(s)
            for copy in leg1_copies(s):
                copy.start()
            sent_a(s)

        @pl.when((s >= 1) & (s < steps + 1))
        def _():
            forward(s - 1)

        @pl.when(s >= 2)
        def _():
            finish(s - 2)

        @pl.when(s + AHEAD < steps)
        def _():
            send_a(s + AHEAD)
        return carry

    lax.fori_loop(0, steps + 2, step, 0)
    for j in range(B_PIECES):
        b_copy(j).wait_send()


def _product(a_rows, b_rows, chunk):
    rows = a_rows.shape[0]
    half_k, cols = b_rows.shape
    steps = rows // chunk
    nt, kt = cols // N_TILES, 2 * half_k // SLICES
    sem = pltpu.SemaphoreType.DMA
    hbm = pl.BlockSpec(memory_space=pl.ANY)
    outs = pl.pallas_call(
        functools.partial(_kernel, chunk),
        out_shape=(
            pltpu.VMEM((rows, cols), jnp.bfloat16),
            jax.ShapeDtypeStruct((half_k, cols), jnp.bfloat16),
            jax.ShapeDtypeStruct((3, rows, 2 * half_k), jnp.bfloat16),
        ),
        in_specs=[hbm] * 2,
        out_specs=(pl.BlockSpec(memory_space=pltpu.VMEM),) + (hbm,) * 2,
        scratch_shapes=[
            pltpu.VMEM((SLICES, 4 * chunk, kt), jnp.bfloat16),
            pltpu.VMEM((SLOTS, kt, nt), jnp.bfloat16),
            pltpu.VMEM((BUFS, 4 * chunk, cols), jnp.float32),
            pltpu.VMEM((RING, 2, chunk, cols), jnp.float32),
            pltpu.VMEM((RING, chunk, cols), jnp.float32),
            sem((B_PIECES,)), sem((B_PIECES,)),
            sem((steps, SLICES, 3)), sem((steps, SLICES, 3)),
            sem((steps, 2)), sem((steps, 2)), sem((steps, 2)), sem((steps, 2)),
            sem((2, 7)), sem((SLOTS,)),
        ],
        compiler_params=pltpu.CompilerParams(
            collective_id=0, has_side_effects=True, vmem_limit_bytes=56 << 20),
    )(a_rows, b_rows)
    return outs[0]


def solution(mesh):
    spec = P(("mp", "dp"), None)

    def local(a_rows, b_rows):
        return _product(a_rows, b_rows, min(64, a_rows.shape[0] // 4))

    return jax.shard_map(local, mesh=mesh, in_specs=(spec, spec), out_specs=spec, check_vma=False)
```

```python
import functools

import jax
import jax.numpy as jnp
from jax import lax
from jax.experimental import pallas as pl
from jax.experimental.pallas import tpu as pltpu
from jax.sharding import PartitionSpec as P

MESH = pl.DeviceIdType.MESH
N_TILES = 8
SLICES = 4
SLOTS = 4
AHEAD = 2
BUFS = 3
RING = 4
B_PIECES = 8


def _kernel(chunk, a_ref, b_ref, c_ref, b_par, a_in,
            a_v, b_v, acc, leg1, leg2, stage,
            bx_send, bx_recv, a_send, a_recv, l1_send, l1_recv, l2_send, l2_recv,
            a_sem, b_sem, stage_sem, diag_sem):
    rows = a_ref.shape[0]
    half_k, cols = b_ref.shape
    chip_k = 2 * half_k
    steps = rows // chunk
    half = chunk // 2
    nt = cols // N_TILES
    kt = chip_k // SLICES
    own_slices = SLICES // 2

    mp = lax.axis_index("mp")
    dp = lax.axis_index("dp")
    core = lax.rem(dp, 2)
    xx = dp // 2
    x_peer = (mp, (1 - xx) * 2 + core)
    y_peer = (1 - mp, dp)
    partner = (mp, xx * 2 + 1 - core)

    def chunk_rows(t):
        return pl.ds(pl.multiple_of(t * chunk, chunk), chunk)

    def slice_start(q):
        h = q // own_slices
        side = core + h - 2 * core * h
        return side * half_k + lax.rem(q, own_slices) * kt

    piece = half_k // B_PIECES

    def b_copy(j):
        span = pl.ds(j * piece, piece)
        return pltpu.make_async_remote_copy(
            src_ref=b_ref.at[span], dst_ref=b_par.at[span],
            send_sem=bx_send.at[j], recv_sem=bx_recv.at[j],
            device_id=partner, device_id_type=MESH)

    def a_place(q, slot):
        is_x = 1 - slot // 2
        is_y = (slot + 1) // 2
        to_mp = mp + is_y * (1 - 2 * mp)
        to_x = xx + is_x * (1 - 2 * xx)
        part = pl.multiple_of(slice_start(q), kt)
        start = pl.multiple_of((to_mp * 2 + to_x) * chip_k + part, kt)
        return part, start, (to_mp, to_x * 2 + core)

    def a_copy_to(t, q, slot, src=None):
        part, start, peer = a_place(q, slot)
        return pltpu.make_async_remote_copy(
            src_ref=a_ref.at[chunk_rows(t), pl.ds(start, kt)] if src is None else src,
            dst_ref=a_in.at[slot, chunk_rows(t), pl.ds(part, kt)],
            send_sem=a_send.at[t, q, slot], recv_sem=a_recv.at[t, q, slot],
            device_id=peer, device_id_type=MESH)

    def a_copy(t, q, order):
        return a_copy_to(t, q, 2 if order == 2 else (core if order == 0 else 1 - core))

    def send_a(t, first=0):
        def body(q, carry):
            for order in range(3):
                a_copy(t, q, order).start()
            return carry
        lax.fori_loop(first, SLICES, body, 0)

    def sent_a(t):
        def body(q, carry):
            for order in range(3):
                a_copy(t, q, order).wait_send()
            return carry
        lax.fori_loop(0, SLICES, body, 0)

    def b_tile(src, q, n, slot):
        return pltpu.make_async_copy(
            src.at[pl.ds(pl.multiple_of(lax.rem(q, own_slices) * kt, kt), kt),
                   pl.ds(pl.multiple_of(n * nt, nt), nt)],
            b_v.at[slot], b_sem.at[slot])

    def load_tile(q, n, slot):
        @pl.when(q < own_slices)
        def _():
            b_tile(b_ref, q, n, slot).start()

        @pl.when(q >= own_slices)
        def _():
            b_tile(b_par, q, n, slot).start()

    def staged(slot):
        start = a_place(0, slot)[1]
        return pltpu.make_async_copy(
            a_ref.at[chunk_rows(0), pl.ds(start, kt)], stage.at[slot], stage_sem.at[slot])

    def send_first(slot):
        @pl.when(core == 0)
        def _():
            staged(slot).wait()
            a_copy_to(0, 0, slot, stage.at[slot]).start()

        @pl.when(core == 1)
        def _():
            a_copy_to(0, 0, slot).start()

    @pl.when(core == 0)
    def _():
        for slot in (0, 2, 1):
            staged(slot).start()

    barrier = pltpu.get_barrier_semaphore()
    for peer in (x_peer, y_peer, partner):
        pl.semaphore_signal(barrier, inc=1, device_id=peer, device_id_type=MESH)
    pl.semaphore_wait(barrier, 3)
    pl.semaphore_signal(diag_sem, inc=1, device_id=y_peer, device_id_type=MESH)
    send_first(0)
    send_first(2)
    pl.semaphore_wait(diag_sem, 1)
    send_first(1)
    send_a(0, 1)
    for t in range(1, AHEAD):
        send_a(t)
    for j in range(B_PIECES):
        b_copy(j).start()
    for slot in range(SLOTS):
        b_tile(b_ref, 0, slot, slot).start()

    sources = [(0, half, 0), (1, half, 0), (2, half, 0), (0, half, half), (1, half, half), (2, half, half)]

    def a_loads(t, q):
        part = slice_start(q)
        mine = pl.multiple_of((mp * 2 + xx) * chip_k + part, kt)
        loads = [pltpu.make_async_copy(
            a_ref.at[chunk_rows(t), pl.ds(mine, kt)], a_v.at[q, pl.ds(0, chunk)],
            a_sem.at[lax.rem(q, 2), 6])]
        for i, (slot, size, off) in enumerate(sources):
            span = pl.ds(pl.multiple_of(t * chunk + off, half), half)
            loads.append(pltpu.make_async_copy(
                a_in.at[slot, span, pl.ds(pl.multiple_of(part, kt), kt)],
                a_v.at[q, pl.ds(chunk + i * half, half)], a_sem.at[lax.rem(q, 2), i]))
        return loads

    def leg1_copies(t):
        buf = lax.rem(t, BUFS)
        return [pltpu.make_async_remote_copy(
            src_ref=acc.at[buf, pl.ds(start, chunk)], dst_ref=leg1.at[lax.rem(t, RING), i],
            send_sem=l1_send.at[t, i], recv_sem=l1_recv.at[t, i],
            device_id=peer, device_id_type=MESH)
            for i, (start, peer) in enumerate(((chunk, x_peer), (chunk + 4 * half, y_peer)))]

    def leg2_copies(t):
        buf = lax.rem(t, BUFS)
        return [pltpu.make_async_remote_copy(
            src_ref=acc.at[buf, pl.ds(chunk + (2 + i) * half, half)],
            dst_ref=leg2.at[lax.rem(t, RING), pl.ds(i * half, half)],
            send_sem=l2_send.at[t, i], recv_sem=l2_recv.at[t, i],
            device_id=peer, device_id_type=MESH)
            for i, peer in enumerate((y_peer, x_peer))]

    def product(t):
        buf = lax.rem(t, BUFS)
        acc[buf] = jnp.zeros(acc.shape[1:], acc.dtype)

        def fetch(q):
            for order in range(3):
                a_copy(t, q, order).wait_recv()
            for load in a_loads(t, q):
                load.start()

        fetch(0)

        def one_slice(q, carry):
            @pl.when(q < SLICES - 1)
            def _():
                fetch(q + 1)

            @pl.when((t == 0) & (q >= own_slices - 1) & (q < SLICES - 1))
            def _():
                def body(j, c):
                    b_copy(j).wait_recv()
                    return c
                per = B_PIECES // own_slices
                lax.fori_loop((q - own_slices + 1) * per, (q - own_slices + 2) * per, body, 0)

            for load in a_loads(t, q):
                load.wait()

            def columns(m, c):
                for slot in range(SLOTS):
                    n = m * SLOTS + slot
                    b_tile(b_ref, q, n, slot).wait()
                    acc[buf, :, pl.ds(pl.multiple_of(n * nt, nt), nt)] += jnp.dot(
                        a_v[q], b_v[slot], preferred_element_type=jnp.float32)
                    later = m + 1
                    wraps = later // (N_TILES // SLOTS)

                    @pl.when((t < steps - 1) | (q < SLICES - 1) | (wraps == 0))
                    def _():
                        load_tile(lax.rem(q + wraps, SLICES),
                                  (later - wraps * (N_TILES // SLOTS)) * SLOTS + slot, slot)
                return c

            lax.fori_loop(0, N_TILES // SLOTS, columns, 0)
            return carry

        lax.fori_loop(0, SLICES, one_slice, 0)

    def forward(t):
        for copy in leg1_copies(t):
            copy.wait_recv()
        buf, slot = lax.rem(t, BUFS), lax.rem(t, RING)
        for i in range(2):
            acc[buf, pl.ds(chunk + (2 + i) * half, half)] += leg1[slot, i, pl.ds((1 - i) * half, half)]
        for copy in leg2_copies(t):
            copy.start()

    def finish(t):
        copies = leg2_copies(t)
        buf, slot = lax.rem(t, BUFS), lax.rem(t, RING)
        for i in range(2):
            copies[i].wait_recv()
            part = pl.ds(i * half, half)
            total = acc[buf, part] + leg1[slot, i, part] + leg2[slot, part]
            c_ref[pl.ds(pl.multiple_of(t * chunk + i * half, half), half)] = total.astype(c_ref.dtype)
        for copy in leg1_copies(t) + leg2_copies(t):
            copy.wait_send()

    def step(s, carry):
        @pl.when(s < steps)
        def _():
            product(s)
            for copy in leg1_copies(s):
                copy.start()
            sent_a(s)

        @pl.when((s >= 1) & (s < steps + 1))
        def _():
            forward(s - 1)

        @pl.when(s >= 2)
        def _():
            finish(s - 2)

        @pl.when(s + AHEAD < steps)
        def _():
            send_a(s + AHEAD)
        return carry

    lax.fori_loop(0, steps + 2, step, 0)
    for j in range(B_PIECES):
        b_copy(j).wait_send()


def _product(a_rows, b_rows, chunk):
    rows = a_rows.shape[0]
    half_k, cols = b_rows.shape
    steps = rows // chunk
    nt, kt = cols // N_TILES, 2 * half_k // SLICES
    sem = pltpu.SemaphoreType.DMA
    hbm = pl.BlockSpec(memory_space=pl.ANY)
    outs = pl.pallas_call(
        functools.partial(_kernel, chunk),
        out_shape=(
            pltpu.VMEM((rows, cols), jnp.bfloat16),
            jax.ShapeDtypeStruct((half_k, cols), jnp.bfloat16),
            jax.ShapeDtypeStruct((3, rows, 2 * half_k), jnp.bfloat16),
        ),
        in_specs=[hbm] * 2,
        out_specs=(pl.BlockSpec(memory_space=pltpu.VMEM),) + (hbm,) * 2,
        scratch_shapes=[
            pltpu.VMEM((SLICES, 4 * chunk, kt), jnp.bfloat16),
            pltpu.VMEM((SLOTS, kt, nt), jnp.bfloat16),
            pltpu.VMEM((BUFS, 4 * chunk, cols), jnp.float32),
            pltpu.VMEM((RING, 2, chunk, cols), jnp.float32),
            pltpu.VMEM((RING, chunk, cols), jnp.float32),
            pltpu.VMEM((3, chunk, kt), jnp.bfloat16),
            sem((B_PIECES,)), sem((B_PIECES,)),
            sem((steps, SLICES, 3)), sem((steps, SLICES, 3)),
            sem((steps, 2)), sem((steps, 2)), sem((steps, 2)), sem((steps, 2)),
            sem((2, 7)), sem((SLOTS,)), sem((3,)), pltpu.SemaphoreType.REGULAR,
        ],
        compiler_params=pltpu.CompilerParams(
            collective_id=0, has_side_effects=True, vmem_limit_bytes=56 << 20),
    )(a_rows, b_rows)
    return outs[0]


def solution(mesh):
    spec = P(("mp", "dp"), None)

    def local(a_rows, b_rows):
        return _product(a_rows, b_rows, min(64, a_rows.shape[0] // 4))

    return jax.shard_map(local, mesh=mesh, in_specs=(spec, spec), out_specs=spec, check_vma=False)
```

```python
import functools

import jax
import jax.numpy as jnp
from jax import lax
from jax.experimental import pallas as pl
from jax.experimental.pallas import tpu as pltpu
from jax.sharding import PartitionSpec as P

MESH = pl.DeviceIdType.MESH
N_TILES = 8
SLICES = 4
SLOTS = 4
AHEAD = 2
BUFS = 3
RING = 4
B_PIECES = 8


def _kernel(chunk, a_ref, b_ref, c_ref, b_par, a_in,
            a_v, b_v, acc, leg1, leg2,
            bx_send, bx_recv, a_send, a_recv, l1_send, l1_recv, l2_send, l2_recv,
            a_sem, b_sem, x_in, y_in, diag_in, core_in):
    rows = a_ref.shape[0]
    half_k, cols = b_ref.shape
    chip_k = 2 * half_k
    steps = rows // chunk
    half = chunk // 2
    nt = cols // N_TILES
    kt = chip_k // SLICES
    own_slices = SLICES // 2

    mp = lax.axis_index("mp")
    dp = lax.axis_index("dp")
    core = lax.rem(dp, 2)
    xx = dp // 2
    x_peer = (mp, (1 - xx) * 2 + core)
    y_peer = (1 - mp, dp)
    partner = (mp, xx * 2 + 1 - core)

    def chunk_rows(t):
        return pl.ds(pl.multiple_of(t * chunk, chunk), chunk)

    def slice_start(q):
        h = q // own_slices
        side = core + h - 2 * core * h
        return side * half_k + lax.rem(q, own_slices) * kt

    piece = half_k // B_PIECES

    def b_copy(j):
        span = pl.ds(j * piece, piece)
        return pltpu.make_async_remote_copy(
            src_ref=b_ref.at[span], dst_ref=b_par.at[span],
            send_sem=bx_send.at[j], recv_sem=bx_recv.at[j],
            device_id=partner, device_id_type=MESH)

    def a_place(q, slot):
        is_x = 1 - slot // 2
        is_y = (slot + 1) // 2
        to_mp = mp + is_y * (1 - 2 * mp)
        to_x = xx + is_x * (1 - 2 * xx)
        part = pl.multiple_of(slice_start(q), kt)
        start = pl.multiple_of((to_mp * 2 + to_x) * chip_k + part, kt)
        return part, start, (to_mp, to_x * 2 + core)

    def a_copy_to(t, q, slot):
        part, start, peer = a_place(q, slot)
        return pltpu.make_async_remote_copy(
            src_ref=a_ref.at[chunk_rows(t), pl.ds(start, kt)],
            dst_ref=a_in.at[slot, chunk_rows(t), pl.ds(part, kt)],
            send_sem=a_send.at[t, q, slot], recv_sem=a_recv.at[t, q, slot],
            device_id=peer, device_id_type=MESH)

    def a_copy(t, q, order):
        return a_copy_to(t, q, 2 if order == 2 else (core if order == 0 else 1 - core))

    def send_a(t, first=0):
        def body(q, carry):
            for order in range(3):
                a_copy(t, q, order).start()
            return carry
        lax.fori_loop(first, SLICES, body, 0)

    def sent_a(t):
        def body(q, carry):
            for order in range(3):
                a_copy(t, q, order).wait_send()
            return carry
        lax.fori_loop(0, SLICES, body, 0)

    def b_tile(src, q, n, slot):
        return pltpu.make_async_copy(
            src.at[pl.ds(pl.multiple_of(lax.rem(q, own_slices) * kt, kt), kt),
                   pl.ds(pl.multiple_of(n * nt, nt), nt)],
            b_v.at[slot], b_sem.at[slot])

    def load_tile(q, n, slot):
        @pl.when(q < own_slices)
        def _():
            b_tile(b_ref, q, n, slot).start()

        @pl.when(q >= own_slices)
        def _():
            b_tile(b_par, q, n, slot).start()

    def signal(semaphore, peer):
        pl.semaphore_signal(semaphore, inc=1, device_id=peer, device_id_type=MESH)

    barrier = pltpu.get_barrier_semaphore()

    @pl.when(xx == 0)
    def _():
        signal(barrier, x_peer)

    @pl.when(mp == 0)
    def _():
        signal(barrier, y_peer)

    @pl.when(core == 0)
    def _():
        signal(barrier, partner)

    @pl.when(xx + mp + core > 0)
    def _():
        pl.semaphore_wait(barrier, xx + mp + core)

    @pl.when(xx == 1)
    def _():
        signal(x_in, x_peer)
        a_copy_to(0, 0, 0).start()

    @pl.when(mp == 1)
    def _():
        signal(y_in, y_peer)
        a_copy_to(0, 0, 2).start()

    @pl.when(core == 1)
    def _():
        signal(core_in, partner)

    @pl.when(xx == 0)
    def _():
        pl.semaphore_wait(x_in, 1)
        a_copy_to(0, 0, 0).start()

    @pl.when(mp == 0)
    def _():
        pl.semaphore_wait(y_in, 1)
        a_copy_to(0, 0, 2).start()

    signal(diag_in, y_peer)
    pl.semaphore_wait(diag_in, 1)
    a_copy_to(0, 0, 1).start()
    send_a(0, 1)
    for t in range(1, AHEAD):
        send_a(t)

    @pl.when(core == 0)
    def _():
        pl.semaphore_wait(core_in, 1)

    for j in range(B_PIECES):
        b_copy(j).start()
    for slot in range(SLOTS):
        b_tile(b_ref, 0, slot, slot).start()

    sources = [(0, half, 0), (1, half, 0), (2, half, 0), (0, half, half), (1, half, half), (2, half, half)]

    def a_loads(t, q):
        part = slice_start(q)
        mine = pl.multiple_of((mp * 2 + xx) * chip_k + part, kt)
        loads = [pltpu.make_async_copy(
            a_ref.at[chunk_rows(t), pl.ds(mine, kt)], a_v.at[q, pl.ds(0, chunk)],
            a_sem.at[lax.rem(q, 2), 6])]
        for i, (slot, size, off) in enumerate(sources):
            span = pl.ds(pl.multiple_of(t * chunk + off, half), half)
            loads.append(pltpu.make_async_copy(
                a_in.at[slot, span, pl.ds(pl.multiple_of(part, kt), kt)],
                a_v.at[q, pl.ds(chunk + i * half, half)], a_sem.at[lax.rem(q, 2), i]))
        return loads

    def leg1_copies(t):
        buf = lax.rem(t, BUFS)
        return [pltpu.make_async_remote_copy(
            src_ref=acc.at[buf, pl.ds(start, chunk)], dst_ref=leg1.at[lax.rem(t, RING), i],
            send_sem=l1_send.at[t, i], recv_sem=l1_recv.at[t, i],
            device_id=peer, device_id_type=MESH)
            for i, (start, peer) in enumerate(((chunk, x_peer), (chunk + 4 * half, y_peer)))]

    def leg2_copies(t):
        buf = lax.rem(t, BUFS)
        return [pltpu.make_async_remote_copy(
            src_ref=acc.at[buf, pl.ds(chunk + (2 + i) * half, half)],
            dst_ref=leg2.at[lax.rem(t, RING), pl.ds(i * half, half)],
            send_sem=l2_send.at[t, i], recv_sem=l2_recv.at[t, i],
            device_id=peer, device_id_type=MESH)
            for i, peer in enumerate((y_peer, x_peer))]

    def product(t):
        buf = lax.rem(t, BUFS)
        acc[buf] = jnp.zeros(acc.shape[1:], acc.dtype)

        def fetch(q):
            for order in range(3):
                a_copy(t, q, order).wait_recv()
            for load in a_loads(t, q):
                load.start()

        fetch(0)

        def one_slice(q, carry):
            @pl.when(q < SLICES - 1)
            def _():
                fetch(q + 1)

            @pl.when((t == 0) & (q >= own_slices - 1) & (q < SLICES - 1))
            def _():
                def body(j, c):
                    b_copy(j).wait_recv()
                    return c
                per = B_PIECES // own_slices
                lax.fori_loop((q - own_slices + 1) * per, (q - own_slices + 2) * per, body, 0)

            for load in a_loads(t, q):
                load.wait()

            def columns(m, c):
                for slot in range(SLOTS):
                    n = m * SLOTS + slot
                    b_tile(b_ref, q, n, slot).wait()
                    acc[buf, :, pl.ds(pl.multiple_of(n * nt, nt), nt)] += jnp.dot(
                        a_v[q], b_v[slot], preferred_element_type=jnp.float32)
                    later = m + 1
                    wraps = later // (N_TILES // SLOTS)

                    @pl.when((t < steps - 1) | (q < SLICES - 1) | (wraps == 0))
                    def _():
                        load_tile(lax.rem(q + wraps, SLICES),
                                  (later - wraps * (N_TILES // SLOTS)) * SLOTS + slot, slot)
                return c

            lax.fori_loop(0, N_TILES // SLOTS, columns, 0)
            return carry

        lax.fori_loop(0, SLICES, one_slice, 0)

    def forward(t):
        for copy in leg1_copies(t):
            copy.wait_recv()
        buf, slot = lax.rem(t, BUFS), lax.rem(t, RING)
        for i in range(2):
            acc[buf, pl.ds(chunk + (2 + i) * half, half)] += leg1[slot, i, pl.ds((1 - i) * half, half)]
        for copy in leg2_copies(t):
            copy.start()

    def finish(t):
        copies = leg2_copies(t)
        buf, slot = lax.rem(t, BUFS), lax.rem(t, RING)
        for i in range(2):
            copies[i].wait_recv()
            part = pl.ds(i * half, half)
            total = acc[buf, part] + leg1[slot, i, part] + leg2[slot, part]
            c_ref[pl.ds(pl.multiple_of(t * chunk + i * half, half), half)] = total.astype(c_ref.dtype)
        for copy in leg1_copies(t) + leg2_copies(t):
            copy.wait_send()

    def step(s, carry):
        @pl.when(s < steps)
        def _():
            product(s)
            for copy in leg1_copies(s):
                copy.start()
            sent_a(s)

        @pl.when((s >= 1) & (s < steps + 1))
        def _():
            forward(s - 1)

        @pl.when(s >= 2)
        def _():
            finish(s - 2)

        @pl.when(s + AHEAD < steps)
        def _():
            send_a(s + AHEAD)
        return carry

    lax.fori_loop(0, steps + 2, step, 0)
    for j in range(B_PIECES):
        b_copy(j).wait_send()


def _product(a_rows, b_rows, chunk):
    rows = a_rows.shape[0]
    half_k, cols = b_rows.shape
    steps = rows // chunk
    nt, kt = cols // N_TILES, 2 * half_k // SLICES
    sem = pltpu.SemaphoreType.DMA
    hbm = pl.BlockSpec(memory_space=pl.ANY)
    outs = pl.pallas_call(
        functools.partial(_kernel, chunk),
        out_shape=(
            pltpu.VMEM((rows, cols), jnp.bfloat16),
            jax.ShapeDtypeStruct((half_k, cols), jnp.bfloat16),
            jax.ShapeDtypeStruct((3, rows, 2 * half_k), jnp.bfloat16),
        ),
        in_specs=[hbm] * 2,
        out_specs=(pl.BlockSpec(memory_space=pltpu.VMEM),) + (hbm,) * 2,
        scratch_shapes=[
            pltpu.VMEM((SLICES, 4 * chunk, kt), jnp.bfloat16),
            pltpu.VMEM((SLOTS, kt, nt), jnp.bfloat16),
            pltpu.VMEM((BUFS, 4 * chunk, cols), jnp.float32),
            pltpu.VMEM((RING, 2, chunk, cols), jnp.float32),
            pltpu.VMEM((RING, chunk, cols), jnp.float32),
            sem((B_PIECES,)), sem((B_PIECES,)),
            sem((steps, SLICES, 3)), sem((steps, SLICES, 3)),
            sem((steps, 2)), sem((steps, 2)), sem((steps, 2)), sem((steps, 2)),
            sem((2, 7)), sem((SLOTS,)), *[pltpu.SemaphoreType.REGULAR] * 4,
        ],
        compiler_params=pltpu.CompilerParams(
            collective_id=0, has_side_effects=True, vmem_limit_bytes=56 << 20),
    )(a_rows, b_rows)
    return outs[0]


def solution(mesh):
    spec = P(("mp", "dp"), None)

    def local(a_rows, b_rows):
        return _product(a_rows, b_rows, min(64, a_rows.shape[0] // 4))

    return jax.shard_map(local, mesh=mesh, in_specs=(spec, spec), out_specs=spec, check_vma=False)
```

```python
import functools

import jax
import jax.numpy as jnp
from jax import lax
from jax.experimental import pallas as pl
from jax.experimental.pallas import tpu as pltpu
from jax.sharding import PartitionSpec as P

MESH = pl.DeviceIdType.MESH
N_TILES = 8
SLICES = 4
SLOTS = 4
AHEAD = 2
BUFS = 3
RING = 4
B_PIECES = 8


def _kernel(chunk, a_ref, b_ref, c_ref, b_par, a_in,
            a_v, b_v, acc, leg1, leg2,
            bx_send, bx_recv, a_send, a_recv, l1_send, l1_recv, l2_send, l2_recv,
            a_sem, b_sem, x_in, y_in, diag_in, core_in):
    rows = a_ref.shape[0]
    half_k, cols = b_ref.shape
    chip_k = 2 * half_k
    steps = rows // chunk
    half = chunk // 2
    nt = cols // N_TILES
    kt = chip_k // SLICES
    own_slices = SLICES // 2

    mp = lax.axis_index("mp")
    dp = lax.axis_index("dp")
    core = lax.rem(dp, 2)
    xx = dp // 2
    x_peer = (mp, (1 - xx) * 2 + core)
    y_peer = (1 - mp, dp)
    partner = (mp, xx * 2 + 1 - core)

    def chunk_rows(t):
        return pl.ds(pl.multiple_of(t * chunk, chunk), chunk)

    def slice_start(q):
        h = q // own_slices
        side = core + h - 2 * core * h
        return side * half_k + lax.rem(q, own_slices) * kt

    piece = half_k // B_PIECES

    def b_copy(j):
        span = pl.ds(j * piece, piece)
        return pltpu.make_async_remote_copy(
            src_ref=b_ref.at[span], dst_ref=b_par.at[span],
            send_sem=bx_send.at[j], recv_sem=bx_recv.at[j],
            device_id=partner, device_id_type=MESH)

    def a_place(q, slot):
        is_x = 1 - slot // 2
        is_y = (slot + 1) // 2
        to_mp = mp + is_y * (1 - 2 * mp)
        to_x = xx + is_x * (1 - 2 * xx)
        part = pl.multiple_of(slice_start(q), kt)
        start = pl.multiple_of((to_mp * 2 + to_x) * chip_k + part, kt)
        return part, start, (to_mp, to_x * 2 + core)

    def a_copy_to(t, q, slot):
        part, start, peer = a_place(q, slot)
        return pltpu.make_async_remote_copy(
            src_ref=a_ref.at[chunk_rows(t), pl.ds(start, kt)],
            dst_ref=a_in.at[slot, chunk_rows(t), pl.ds(part, kt)],
            send_sem=a_send.at[t, q, slot], recv_sem=a_recv.at[t, q, slot],
            device_id=peer, device_id_type=MESH)

    def a_copy(t, q, order):
        return a_copy_to(t, q, 2 if order == 2 else (core if order == 0 else 1 - core))

    def send_a(t, first=0):
        def body(q, carry):
            for order in range(3):
                a_copy(t, q, order).start()
            return carry
        lax.fori_loop(first, SLICES, body, 0)

    def sent_a(t):
        def body(q, carry):
            a_copy_to(t, q, 1).wait_send()

            @pl.when((t > 0) | (q > 0) | (core == 0))
            def _():
                for slot in (0, 2):
                    a_copy_to(t, q, slot).wait_send()
            return carry
        lax.fori_loop(0, SLICES, body, 0)

    def b_tile(src, q, n, slot):
        return pltpu.make_async_copy(
            src.at[pl.ds(pl.multiple_of(lax.rem(q, own_slices) * kt, kt), kt),
                   pl.ds(pl.multiple_of(n * nt, nt), nt)],
            b_v.at[slot], b_sem.at[slot])

    def load_tile(q, n, slot):
        @pl.when(q < own_slices)
        def _():
            b_tile(b_ref, q, n, slot).start()

        @pl.when(q >= own_slices)
        def _():
            b_tile(b_par, q, n, slot).start()

    def signal(semaphore, peer):
        pl.semaphore_signal(semaphore, inc=1, device_id=peer, device_id_type=MESH)

    barrier = pltpu.get_barrier_semaphore()

    @pl.when(xx == 0)
    def _():
        signal(barrier, x_peer)

    @pl.when(mp == 0)
    def _():
        signal(barrier, y_peer)

    @pl.when(core == 1)
    def _():
        signal(barrier, partner)

    @pl.when(xx + mp + 1 - core > 0)
    def _():
        pl.semaphore_wait(barrier, xx + mp + 1 - core)

    @pl.when(xx == 1)
    def _():
        signal(x_in, x_peer)
        a_copy_to(0, 0, 0).start()

    @pl.when(mp == 1)
    def _():
        signal(y_in, y_peer)
        a_copy_to(0, 0, 2).start()

    @pl.when(core == 0)
    def _():
        signal(core_in, partner)

    @pl.when(xx == 0)
    def _():
        pl.semaphore_wait(x_in, 1)
        a_copy_to(0, 0, 0).start()

    @pl.when(mp == 0)
    def _():
        pl.semaphore_wait(y_in, 1)
        a_copy_to(0, 0, 2).start()

    signal(diag_in, y_peer)

    @pl.when(core == 1)
    def _():
        for slot in (0, 2):
            a_copy_to(0, 0, slot).wait_send()

    pl.semaphore_wait(diag_in, 1)
    a_copy_to(0, 0, 1).start()
    send_a(0, 1)
    for t in range(1, AHEAD):
        send_a(t)

    @pl.when(core == 1)
    def _():
        pl.semaphore_wait(core_in, 1)

    for j in range(B_PIECES):
        b_copy(j).start()
    for slot in range(SLOTS):
        b_tile(b_ref, 0, slot, slot).start()

    sources = [(0, half, 0), (1, half, 0), (2, half, 0), (0, half, half), (1, half, half), (2, half, half)]

    def a_loads(t, q):
        part = slice_start(q)
        mine = pl.multiple_of((mp * 2 + xx) * chip_k + part, kt)
        loads = [pltpu.make_async_copy(
            a_ref.at[chunk_rows(t), pl.ds(mine, kt)], a_v.at[q, pl.ds(0, chunk)],
            a_sem.at[lax.rem(q, 2), 6])]
        for i, (slot, size, off) in enumerate(sources):
            span = pl.ds(pl.multiple_of(t * chunk + off, half), half)
            loads.append(pltpu.make_async_copy(
                a_in.at[slot, span, pl.ds(pl.multiple_of(part, kt), kt)],
                a_v.at[q, pl.ds(chunk + i * half, half)], a_sem.at[lax.rem(q, 2), i]))
        return loads

    def leg1_copies(t):
        buf = lax.rem(t, BUFS)
        return [pltpu.make_async_remote_copy(
            src_ref=acc.at[buf, pl.ds(start, chunk)], dst_ref=leg1.at[lax.rem(t, RING), i],
            send_sem=l1_send.at[t, i], recv_sem=l1_recv.at[t, i],
            device_id=peer, device_id_type=MESH)
            for i, (start, peer) in enumerate(((chunk, x_peer), (chunk + 4 * half, y_peer)))]

    def leg2_copies(t):
        buf = lax.rem(t, BUFS)
        return [pltpu.make_async_remote_copy(
            src_ref=acc.at[buf, pl.ds(chunk + (2 + i) * half, half)],
            dst_ref=leg2.at[lax.rem(t, RING), pl.ds(i * half, half)],
            send_sem=l2_send.at[t, i], recv_sem=l2_recv.at[t, i],
            device_id=peer, device_id_type=MESH)
            for i, peer in enumerate((y_peer, x_peer))]

    def product(t):
        buf = lax.rem(t, BUFS)
        acc[buf] = jnp.zeros(acc.shape[1:], acc.dtype)

        def fetch(q):
            for order in range(3):
                a_copy(t, q, order).wait_recv()
            for load in a_loads(t, q):
                load.start()

        fetch(0)

        def one_slice(q, carry):
            @pl.when(q < SLICES - 1)
            def _():
                fetch(q + 1)

            @pl.when((t == 0) & (q >= own_slices - 1) & (q < SLICES - 1))
            def _():
                def body(j, c):
                    b_copy(j).wait_recv()
                    return c
                per = B_PIECES // own_slices
                lax.fori_loop((q - own_slices + 1) * per, (q - own_slices + 2) * per, body, 0)

            for load in a_loads(t, q):
                load.wait()

            def columns(m, c):
                for slot in range(SLOTS):
                    n = m * SLOTS + slot
                    b_tile(b_ref, q, n, slot).wait()
                    acc[buf, :, pl.ds(pl.multiple_of(n * nt, nt), nt)] += jnp.dot(
                        a_v[q], b_v[slot], preferred_element_type=jnp.float32)
                    later = m + 1
                    wraps = later // (N_TILES // SLOTS)

                    @pl.when((t < steps - 1) | (q < SLICES - 1) | (wraps == 0))
                    def _():
                        load_tile(lax.rem(q + wraps, SLICES),
                                  (later - wraps * (N_TILES // SLOTS)) * SLOTS + slot, slot)
                return c

            lax.fori_loop(0, N_TILES // SLOTS, columns, 0)
            return carry

        lax.fori_loop(0, SLICES, one_slice, 0)

    def forward(t):
        for copy in leg1_copies(t):
            copy.wait_recv()
        buf, slot = lax.rem(t, BUFS), lax.rem(t, RING)
        for i in range(2):
            acc[buf, pl.ds(chunk + (2 + i) * half, half)] += leg1[slot, i, pl.ds((1 - i) * half, half)]
        for copy in leg2_copies(t):
            copy.start()

    def finish(t):
        copies = leg2_copies(t)
        buf, slot = lax.rem(t, BUFS), lax.rem(t, RING)
        for i in range(2):
            copies[i].wait_recv()
            part = pl.ds(i * half, half)
            total = acc[buf, part] + leg1[slot, i, part] + leg2[slot, part]
            c_ref[pl.ds(pl.multiple_of(t * chunk + i * half, half), half)] = total.astype(c_ref.dtype)
        for copy in leg1_copies(t) + leg2_copies(t):
            copy.wait_send()

    def step(s, carry):
        @pl.when(s < steps)
        def _():
            product(s)
            for copy in leg1_copies(s):
                copy.start()
            sent_a(s)

        @pl.when((s >= 1) & (s < steps + 1))
        def _():
            forward(s - 1)

        @pl.when(s >= 2)
        def _():
            finish(s - 2)

        @pl.when(s + AHEAD < steps)
        def _():
            send_a(s + AHEAD)
        return carry

    lax.fori_loop(0, steps + 2, step, 0)
    for j in range(B_PIECES):
        b_copy(j).wait_send()


def _product(a_rows, b_rows, chunk):
    rows = a_rows.shape[0]
    half_k, cols = b_rows.shape
    steps = rows // chunk
    nt, kt = cols // N_TILES, 2 * half_k // SLICES
    sem = pltpu.SemaphoreType.DMA
    hbm = pl.BlockSpec(memory_space=pl.ANY)
    outs = pl.pallas_call(
        functools.partial(_kernel, chunk),
        out_shape=(
            pltpu.VMEM((rows, cols), jnp.bfloat16),
            jax.ShapeDtypeStruct((half_k, cols), jnp.bfloat16),
            jax.ShapeDtypeStruct((3, rows, 2 * half_k), jnp.bfloat16),
        ),
        in_specs=[hbm] * 2,
        out_specs=(pl.BlockSpec(memory_space=pltpu.VMEM),) + (hbm,) * 2,
        scratch_shapes=[
            pltpu.VMEM((SLICES, 4 * chunk, kt), jnp.bfloat16),
            pltpu.VMEM((SLOTS, kt, nt), jnp.bfloat16),
            pltpu.VMEM((BUFS, 4 * chunk, cols), jnp.float32),
            pltpu.VMEM((RING, 2, chunk, cols), jnp.float32),
            pltpu.VMEM((RING, chunk, cols), jnp.float32),
            sem((B_PIECES,)), sem((B_PIECES,)),
            sem((steps, SLICES, 3)), sem((steps, SLICES, 3)),
            sem((steps, 2)), sem((steps, 2)), sem((steps, 2)), sem((steps, 2)),
            sem((2, 7)), sem((SLOTS,)), *[pltpu.SemaphoreType.REGULAR] * 4,
        ],
        compiler_params=pltpu.CompilerParams(
            collective_id=0, has_side_effects=True, vmem_limit_bytes=56 << 20),
    )(a_rows, b_rows)
    return outs[0]


def solution(mesh):
    spec = P(("mp", "dp"), None)

    def local(a_rows, b_rows):
        return _product(a_rows, b_rows, min(64, a_rows.shape[0] // 4))

    return jax.shard_map(local, mesh=mesh, in_specs=(spec, spec), out_specs=spec, check_vma=False)
```

```python
import functools

import jax
import jax.numpy as jnp
from jax import lax
from jax.experimental import pallas as pl
from jax.experimental.pallas import tpu as pltpu
from jax.sharding import PartitionSpec as P

MESH = pl.DeviceIdType.MESH
N_TILES = 8
SLICES = 4
SLOTS = 4
AHEAD = 2
BUFS = 3
RING = 4
B_PIECES = 8


def _kernel(chunk, a_ref, b_ref, c_ref, b_par, a_in,
            a_v, b_v, acc, leg1, leg2,
            bx_send, bx_recv, a_send, a_recv, l1_send, l1_recv, l2_send, l2_recv,
            a_sem, b_sem, x_in, y_in, diag_in, core_in):
    rows = a_ref.shape[0]
    half_k, cols = b_ref.shape
    chip_k = 2 * half_k
    steps = rows // chunk
    half = chunk // 2
    nt = cols // N_TILES
    kt = chip_k // SLICES
    own_slices = SLICES // 2

    mp = lax.axis_index("mp")
    dp = lax.axis_index("dp")
    core = lax.rem(dp, 2)
    xx = dp // 2
    x_peer = (mp, (1 - xx) * 2 + core)
    y_peer = (1 - mp, dp)
    partner = (mp, xx * 2 + 1 - core)

    def chunk_rows(t):
        return pl.ds(pl.multiple_of(t * chunk, chunk), chunk)

    def slice_start(q):
        h = q // own_slices
        side = core + h - 2 * core * h
        return side * half_k + lax.rem(q, own_slices) * kt

    piece = half_k // B_PIECES

    def b_copy(j):
        span = pl.ds(j * piece, piece)
        return pltpu.make_async_remote_copy(
            src_ref=b_ref.at[span], dst_ref=b_par.at[span],
            send_sem=bx_send.at[j], recv_sem=bx_recv.at[j],
            device_id=partner, device_id_type=MESH)

    def a_place(q, slot):
        is_x = 1 - slot // 2
        is_y = (slot + 1) // 2
        to_mp = mp + is_y * (1 - 2 * mp)
        to_x = xx + is_x * (1 - 2 * xx)
        part = pl.multiple_of(slice_start(q), kt)
        start = pl.multiple_of((to_mp * 2 + to_x) * chip_k + part, kt)
        return part, start, (to_mp, to_x * 2 + core)

    def a_copy_to(t, q, slot):
        part, start, peer = a_place(q, slot)
        return pltpu.make_async_remote_copy(
            src_ref=a_ref.at[chunk_rows(t), pl.ds(start, kt)],
            dst_ref=a_in.at[slot, chunk_rows(t), pl.ds(part, kt)],
            send_sem=a_send.at[t, q, slot], recv_sem=a_recv.at[t, q, slot],
            device_id=peer, device_id_type=MESH)

    def a_copy(t, q, order):
        return a_copy_to(t, q, 2 if order == 2 else (core if order == 0 else 1 - core))

    def send_a(t, first=0):
        def body(q, carry):
            for order in range(3):
                a_copy(t, q, order).start()
            return carry
        lax.fori_loop(first, SLICES, body, 0)

    def sent_a(t):
        def body(q, carry):
            @pl.when((t > 0) | (q > 0) | (core == 0))
            def _():
                for slot in (0, 1):
                    a_copy_to(t, q, slot).wait_send()

            @pl.when((t > 0) | (q > 1) | (core == 0))
            def _():
                a_copy_to(t, q, 2).wait_send()
            return carry
        lax.fori_loop(0, SLICES, body, 0)

    def b_tile(src, q, n, slot):
        return pltpu.make_async_copy(
            src.at[pl.ds(pl.multiple_of(lax.rem(q, own_slices) * kt, kt), kt),
                   pl.ds(pl.multiple_of(n * nt, nt), nt)],
            b_v.at[slot], b_sem.at[slot])

    def load_tile(q, n, slot):
        @pl.when(q < own_slices)
        def _():
            b_tile(b_ref, q, n, slot).start()

        @pl.when(q >= own_slices)
        def _():
            b_tile(b_par, q, n, slot).start()

    def signal(semaphore, peer):
        pl.semaphore_signal(semaphore, inc=1, device_id=peer, device_id_type=MESH)

    barrier = pltpu.get_barrier_semaphore()

    @pl.when(xx == 0)
    def _():
        signal(barrier, x_peer)

    @pl.when(mp == 0)
    def _():
        signal(barrier, y_peer)

    @pl.when(core == 1)
    def _():
        signal(barrier, partner)

    @pl.when(xx + mp + 1 - core > 0)
    def _():
        pl.semaphore_wait(barrier, xx + mp + 1 - core)

    @pl.when(xx == 1)
    def _():
        signal(x_in, x_peer)
        a_copy_to(0, 0, 0).start()

    @pl.when(mp == 1)
    def _():
        signal(y_in, y_peer)
        a_copy_to(0, 0, 2).start()

    @pl.when(core == 0)
    def _():
        signal(core_in, partner)

    @pl.when(xx == 0)
    def _():
        pl.semaphore_wait(x_in, 1)
        a_copy_to(0, 0, 0).start()

    @pl.when(mp == 0)
    def _():
        pl.semaphore_wait(y_in, 1)
        a_copy_to(0, 0, 2).start()

    signal(diag_in, y_peer)

    @pl.when(core == 1)
    def _():
        for slot in (0, 2):
            a_copy_to(0, 0, slot).wait_send()

    pl.semaphore_wait(diag_in, 1)
    a_copy_to(0, 0, 1).start()

    @pl.when(core == 1)
    def _():
        a_copy_to(0, 1, 2).start()
        a_copy_to(0, 0, 1).wait_send()
        a_copy_to(0, 1, 2).wait_send()

    for order in range(2):
        a_copy(0, 1, order).start()

    @pl.when(core == 0)
    def _():
        a_copy_to(0, 1, 2).start()

    send_a(0, 2)
    for t in range(1, AHEAD):
        send_a(t)

    @pl.when(core == 1)
    def _():
        pl.semaphore_wait(core_in, 1)

    for j in range(B_PIECES):
        b_copy(j).start()
    for slot in range(SLOTS):
        b_tile(b_ref, 0, slot, slot).start()

    sources = [(0, half, 0), (1, half, 0), (2, half, 0), (0, half, half), (1, half, half), (2, half, half)]

    def a_loads(t, q):
        part = slice_start(q)
        mine = pl.multiple_of((mp * 2 + xx) * chip_k + part, kt)
        loads = [pltpu.make_async_copy(
            a_ref.at[chunk_rows(t), pl.ds(mine, kt)], a_v.at[q, pl.ds(0, chunk)],
            a_sem.at[lax.rem(q, 2), 6])]
        for i, (slot, size, off) in enumerate(sources):
            span = pl.ds(pl.multiple_of(t * chunk + off, half), half)
            loads.append(pltpu.make_async_copy(
                a_in.at[slot, span, pl.ds(pl.multiple_of(part, kt), kt)],
                a_v.at[q, pl.ds(chunk + i * half, half)], a_sem.at[lax.rem(q, 2), i]))
        return loads

    def leg1_copies(t):
        buf = lax.rem(t, BUFS)
        return [pltpu.make_async_remote_copy(
            src_ref=acc.at[buf, pl.ds(start, chunk)], dst_ref=leg1.at[lax.rem(t, RING), i],
            send_sem=l1_send.at[t, i], recv_sem=l1_recv.at[t, i],
            device_id=peer, device_id_type=MESH)
            for i, (start, peer) in enumerate(((chunk, x_peer), (chunk + 4 * half, y_peer)))]

    def leg2_copies(t):
        buf = lax.rem(t, BUFS)
        return [pltpu.make_async_remote_copy(
            src_ref=acc.at[buf, pl.ds(chunk + (2 + i) * half, half)],
            dst_ref=leg2.at[lax.rem(t, RING), pl.ds(i * half, half)],
            send_sem=l2_send.at[t, i], recv_sem=l2_recv.at[t, i],
            device_id=peer, device_id_type=MESH)
            for i, peer in enumerate((y_peer, x_peer))]

    def product(t):
        buf = lax.rem(t, BUFS)
        acc[buf] = jnp.zeros(acc.shape[1:], acc.dtype)

        def fetch(q):
            for order in range(3):
                a_copy(t, q, order).wait_recv()
            for load in a_loads(t, q):
                load.start()

        fetch(0)

        def one_slice(q, carry):
            @pl.when(q < SLICES - 1)
            def _():
                fetch(q + 1)

            @pl.when((t == 0) & (q >= own_slices - 1) & (q < SLICES - 1))
            def _():
                def body(j, c):
                    b_copy(j).wait_recv()
                    return c
                per = B_PIECES // own_slices
                lax.fori_loop((q - own_slices + 1) * per, (q - own_slices + 2) * per, body, 0)

            for load in a_loads(t, q):
                load.wait()

            def columns(m, c):
                for slot in range(SLOTS):
                    n = m * SLOTS + slot
                    b_tile(b_ref, q, n, slot).wait()
                    acc[buf, :, pl.ds(pl.multiple_of(n * nt, nt), nt)] += jnp.dot(
                        a_v[q], b_v[slot], preferred_element_type=jnp.float32)
                    later = m + 1
                    wraps = later // (N_TILES // SLOTS)

                    @pl.when((t < steps - 1) | (q < SLICES - 1) | (wraps == 0))
                    def _():
                        load_tile(lax.rem(q + wraps, SLICES),
                                  (later - wraps * (N_TILES // SLOTS)) * SLOTS + slot, slot)
                return c

            lax.fori_loop(0, N_TILES // SLOTS, columns, 0)
            return carry

        lax.fori_loop(0, SLICES, one_slice, 0)

    def forward(t):
        for copy in leg1_copies(t):
            copy.wait_recv()
        buf, slot = lax.rem(t, BUFS), lax.rem(t, RING)
        for i in range(2):
            acc[buf, pl.ds(chunk + (2 + i) * half, half)] += leg1[slot, i, pl.ds((1 - i) * half, half)]
        for copy in leg2_copies(t):
            copy.start()

    def finish(t):
        copies = leg2_copies(t)
        buf, slot = lax.rem(t, BUFS), lax.rem(t, RING)
        for i in range(2):
            copies[i].wait_recv()
            part = pl.ds(i * half, half)
            total = acc[buf, part] + leg1[slot, i, part] + leg2[slot, part]
            c_ref[pl.ds(pl.multiple_of(t * chunk + i * half, half), half)] = total.astype(c_ref.dtype)
        for copy in leg1_copies(t) + leg2_copies(t):
            copy.wait_send()

    def step(s, carry):
        @pl.when(s < steps)
        def _():
            product(s)
            for copy in leg1_copies(s):
                copy.start()
            sent_a(s)

        @pl.when((s >= 1) & (s < steps + 1))
        def _():
            forward(s - 1)

        @pl.when(s >= 2)
        def _():
            finish(s - 2)

        @pl.when(s + AHEAD < steps)
        def _():
            send_a(s + AHEAD)
        return carry

    lax.fori_loop(0, steps + 2, step, 0)
    for j in range(B_PIECES):
        b_copy(j).wait_send()


def _product(a_rows, b_rows, chunk):
    rows = a_rows.shape[0]
    half_k, cols = b_rows.shape
    steps = rows // chunk
    nt, kt = cols // N_TILES, 2 * half_k // SLICES
    sem = pltpu.SemaphoreType.DMA
    hbm = pl.BlockSpec(memory_space=pl.ANY)
    outs = pl.pallas_call(
        functools.partial(_kernel, chunk),
        out_shape=(
            pltpu.VMEM((rows, cols), jnp.bfloat16),
            jax.ShapeDtypeStruct((half_k, cols), jnp.bfloat16),
            jax.ShapeDtypeStruct((3, rows, 2 * half_k), jnp.bfloat16),
        ),
        in_specs=[hbm] * 2,
        out_specs=(pl.BlockSpec(memory_space=pltpu.VMEM),) + (hbm,) * 2,
        scratch_shapes=[
            pltpu.VMEM((SLICES, 4 * chunk, kt), jnp.bfloat16),
            pltpu.VMEM((SLOTS, kt, nt), jnp.bfloat16),
            pltpu.VMEM((BUFS, 4 * chunk, cols), jnp.float32),
            pltpu.VMEM((RING, 2, chunk, cols), jnp.float32),
            pltpu.VMEM((RING, chunk, cols), jnp.float32),
            sem((B_PIECES,)), sem((B_PIECES,)),
            sem((steps, SLICES, 3)), sem((steps, SLICES, 3)),
            sem((steps, 2)), sem((steps, 2)), sem((steps, 2)), sem((steps, 2)),
            sem((2, 7)), sem((SLOTS,)), *[pltpu.SemaphoreType.REGULAR] * 4,
        ],
        compiler_params=pltpu.CompilerParams(
            collective_id=0, has_side_effects=True, vmem_limit_bytes=56 << 20),
    )(a_rows, b_rows)
    return outs[0]


def solution(mesh):
    spec = P(("mp", "dp"), None)

    def local(a_rows, b_rows):
        return _product(a_rows, b_rows, min(64, a_rows.shape[0] // 4))

    return jax.shard_map(local, mesh=mesh, in_specs=(spec, spec), out_specs=spec, check_vma=False)
```

```python
import functools

import jax
import jax.numpy as jnp
from jax import lax
from jax.experimental import pallas as pl
from jax.experimental.pallas import tpu as pltpu
from jax.sharding import PartitionSpec as P

MESH = pl.DeviceIdType.MESH
N_TILES = 8
SLICES = 4
SLOTS = 4
AHEAD = 2
BUFS = 3
RING = 4
B_PIECES = 8


def _kernel(chunk, a_ref, b_ref, c_ref, b_par, a_in,
            a_v, b_v, acc, leg1, leg2,
            bx_send, bx_recv, a_send, a_recv, l1_send, l1_recv, l2_send, l2_recv,
            a_sem, b_sem, x_in, y_in, diag_in, core_in):
    rows = a_ref.shape[0]
    half_k, cols = b_ref.shape
    chip_k = 2 * half_k
    steps = rows // chunk
    half = chunk // 2
    nt = cols // N_TILES
    kt = chip_k // SLICES
    own_slices = SLICES // 2

    mp = lax.axis_index("mp")
    dp = lax.axis_index("dp")
    core = lax.rem(dp, 2)
    xx = dp // 2
    x_peer = (mp, (1 - xx) * 2 + core)
    y_peer = (1 - mp, dp)
    partner = (mp, xx * 2 + 1 - core)

    def chunk_rows(t):
        return pl.ds(pl.multiple_of(t * chunk, chunk), chunk)

    def slice_start(q):
        h = q // own_slices
        side = core + h - 2 * core * h
        return side * half_k + lax.rem(q, own_slices) * kt

    piece = half_k // B_PIECES

    def b_copy(j):
        span = pl.ds(j * piece, piece)
        return pltpu.make_async_remote_copy(
            src_ref=b_ref.at[span], dst_ref=b_par.at[span],
            send_sem=bx_send.at[j], recv_sem=bx_recv.at[j],
            device_id=partner, device_id_type=MESH)

    def a_place(q, slot):
        is_x = 1 - slot // 2
        is_y = (slot + 1) // 2
        to_mp = mp + is_y * (1 - 2 * mp)
        to_x = xx + is_x * (1 - 2 * xx)
        part = pl.multiple_of(slice_start(q), kt)
        start = pl.multiple_of((to_mp * 2 + to_x) * chip_k + part, kt)
        return part, start, (to_mp, to_x * 2 + core)

    def a_copy_to(t, q, slot):
        part, start, peer = a_place(q, slot)
        return pltpu.make_async_remote_copy(
            src_ref=a_ref.at[chunk_rows(t), pl.ds(start, kt)],
            dst_ref=a_in.at[slot, chunk_rows(t), pl.ds(part, kt)],
            send_sem=a_send.at[t, q, slot], recv_sem=a_recv.at[t, q, slot],
            device_id=peer, device_id_type=MESH)

    def a_copy(t, q, order):
        return a_copy_to(t, q, 2 if order == 2 else (core if order == 0 else 1 - core))

    def send_a(t, first=0):
        def body(q, carry):
            for order in range(3):
                a_copy(t, q, order).start()
            return carry
        lax.fori_loop(first, SLICES, body, 0)

    def sent_a(t):
        def body(q, carry):
            a_copy_to(t, q, 1).wait_send()

            @pl.when((t > 0) | (q > 0) | (core == 0))
            def _():
                a_copy_to(t, q, 0).wait_send()

            @pl.when((t > 0) | (q > 1) | (core == 0))
            def _():
                a_copy_to(t, q, 2).wait_send()
            return carry
        lax.fori_loop(0, SLICES, body, 0)

    def b_tile(src, q, n, slot):
        return pltpu.make_async_copy(
            src.at[pl.ds(pl.multiple_of(lax.rem(q, own_slices) * kt, kt), kt),
                   pl.ds(pl.multiple_of(n * nt, nt), nt)],
            b_v.at[slot], b_sem.at[slot])

    def load_tile(q, n, slot):
        @pl.when(q < own_slices)
        def _():
            b_tile(b_ref, q, n, slot).start()

        @pl.when(q >= own_slices)
        def _():
            b_tile(b_par, q, n, slot).start()

    def signal(semaphore, peer):
        pl.semaphore_signal(semaphore, inc=1, device_id=peer, device_id_type=MESH)

    barrier = pltpu.get_barrier_semaphore()

    @pl.when(xx == 0)
    def _():
        signal(barrier, x_peer)

    @pl.when(mp == 0)
    def _():
        signal(barrier, y_peer)

    @pl.when(core == 1)
    def _():
        signal(barrier, partner)

    @pl.when(xx + mp + 1 - core > 0)
    def _():
        pl.semaphore_wait(barrier, xx + mp + 1 - core)

    @pl.when(xx == 1)
    def _():
        signal(x_in, x_peer)
        a_copy_to(0, 0, 0).start()

    @pl.when(mp == 1)
    def _():
        signal(y_in, y_peer)
        a_copy_to(0, 0, 2).start()

    @pl.when(core == 0)
    def _():
        signal(core_in, partner)

    @pl.when(xx == 0)
    def _():
        pl.semaphore_wait(x_in, 1)
        a_copy_to(0, 0, 0).start()

    @pl.when(mp == 0)
    def _():
        pl.semaphore_wait(y_in, 1)
        a_copy_to(0, 0, 2).start()

    signal(diag_in, y_peer)

    @pl.when(core == 1)
    def _():
        for slot in (0, 2):
            a_copy_to(0, 0, slot).wait_send()

    pl.semaphore_wait(diag_in, 1)
    a_copy_to(0, 0, 1).start()

    @pl.when(core == 1)
    def _():
        a_copy_to(0, 1, 2).start()
        a_copy_to(0, 1, 2).wait_send()

    for order in range(2):
        a_copy(0, 1, order).start()

    @pl.when(core == 0)
    def _():
        a_copy_to(0, 1, 2).start()

    send_a(0, 2)
    for t in range(1, AHEAD):
        send_a(t)

    @pl.when(core == 1)
    def _():
        pl.semaphore_wait(core_in, 1)

    for j in range(B_PIECES):
        b_copy(j).start()
    for slot in range(SLOTS):
        b_tile(b_ref, 0, slot, slot).start()

    sources = [(0, half, 0), (1, half, 0), (2, half, 0), (0, half, half), (1, half, half), (2, half, half)]

    def a_loads(t, q):
        part = slice_start(q)
        mine = pl.multiple_of((mp * 2 + xx) * chip_k + part, kt)
        loads = [pltpu.make_async_copy(
            a_ref.at[chunk_rows(t), pl.ds(mine, kt)], a_v.at[q, pl.ds(0, chunk)],
            a_sem.at[lax.rem(q, 2), 6])]
        for i, (slot, size, off) in enumerate(sources):
            span = pl.ds(pl.multiple_of(t * chunk + off, half), half)
            loads.append(pltpu.make_async_copy(
                a_in.at[slot, span, pl.ds(pl.multiple_of(part, kt), kt)],
                a_v.at[q, pl.ds(chunk + i * half, half)], a_sem.at[lax.rem(q, 2), i]))
        return loads

    def leg1_copies(t):
        buf = lax.rem(t, BUFS)
        return [pltpu.make_async_remote_copy(
            src_ref=acc.at[buf, pl.ds(start, chunk)], dst_ref=leg1.at[lax.rem(t, RING), i],
            send_sem=l1_send.at[t, i], recv_sem=l1_recv.at[t, i],
            device_id=peer, device_id_type=MESH)
            for i, (start, peer) in enumerate(((chunk, x_peer), (chunk + 4 * half, y_peer)))]

    def leg2_copies(t):
        buf = lax.rem(t, BUFS)
        return [pltpu.make_async_remote_copy(
            src_ref=acc.at[buf, pl.ds(chunk + (2 + i) * half, half)],
            dst_ref=leg2.at[lax.rem(t, RING), pl.ds(i * half, half)],
            send_sem=l2_send.at[t, i], recv_sem=l2_recv.at[t, i],
            device_id=peer, device_id_type=MESH)
            for i, peer in enumerate((y_peer, x_peer))]

    def product(t):
        buf = lax.rem(t, BUFS)
        acc[buf] = jnp.zeros(acc.shape[1:], acc.dtype)

        def fetch(q):
            for order in range(3):
                a_copy(t, q, order).wait_recv()
            for load in a_loads(t, q):
                load.start()

        fetch(0)

        def one_slice(q, carry):
            @pl.when(q < SLICES - 1)
            def _():
                fetch(q + 1)

            @pl.when((t == 0) & (q >= own_slices - 1) & (q < SLICES - 1))
            def _():
                def body(j, c):
                    b_copy(j).wait_recv()
                    return c
                per = B_PIECES // own_slices
                lax.fori_loop((q - own_slices + 1) * per, (q - own_slices + 2) * per, body, 0)

            for load in a_loads(t, q):
                load.wait()

            def columns(m, c):
                for slot in range(SLOTS):
                    n = m * SLOTS + slot
                    b_tile(b_ref, q, n, slot).wait()
                    acc[buf, :, pl.ds(pl.multiple_of(n * nt, nt), nt)] += jnp.dot(
                        a_v[q], b_v[slot], preferred_element_type=jnp.float32)
                    later = m + 1
                    wraps = later // (N_TILES // SLOTS)

                    @pl.when((t < steps - 1) | (q < SLICES - 1) | (wraps == 0))
                    def _():
                        load_tile(lax.rem(q + wraps, SLICES),
                                  (later - wraps * (N_TILES // SLOTS)) * SLOTS + slot, slot)
                return c

            lax.fori_loop(0, N_TILES // SLOTS, columns, 0)
            return carry

        lax.fori_loop(0, SLICES, one_slice, 0)

    def forward(t):
        for copy in leg1_copies(t):
            copy.wait_recv()
        buf, slot = lax.rem(t, BUFS), lax.rem(t, RING)
        for i in range(2):
            acc[buf, pl.ds(chunk + (2 + i) * half, half)] += leg1[slot, i, pl.ds((1 - i) * half, half)]
        for copy in leg2_copies(t):
            copy.start()

    def finish(t):
        copies = leg2_copies(t)
        buf, slot = lax.rem(t, BUFS), lax.rem(t, RING)
        for i in range(2):
            copies[i].wait_recv()
            part = pl.ds(i * half, half)
            total = acc[buf, part] + leg1[slot, i, part] + leg2[slot, part]
            c_ref[pl.ds(pl.multiple_of(t * chunk + i * half, half), half)] = total.astype(c_ref.dtype)
        for copy in leg1_copies(t) + leg2_copies(t):
            copy.wait_send()

    def step(s, carry):
        @pl.when(s < steps)
        def _():
            product(s)
            for copy in leg1_copies(s):
                copy.start()
            sent_a(s)

        @pl.when((s >= 1) & (s < steps + 1))
        def _():
            forward(s - 1)

        @pl.when(s >= 2)
        def _():
            finish(s - 2)

        @pl.when(s + AHEAD < steps)
        def _():
            send_a(s + AHEAD)
        return carry

    lax.fori_loop(0, steps + 2, step, 0)
    for j in range(B_PIECES):
        b_copy(j).wait_send()


def _product(a_rows, b_rows, chunk):
    rows = a_rows.shape[0]
    half_k, cols = b_rows.shape
    steps = rows // chunk
    nt, kt = cols // N_TILES, 2 * half_k // SLICES
    sem = pltpu.SemaphoreType.DMA
    hbm = pl.BlockSpec(memory_space=pl.ANY)
    outs = pl.pallas_call(
        functools.partial(_kernel, chunk),
        out_shape=(
            pltpu.VMEM((rows, cols), jnp.bfloat16),
            jax.ShapeDtypeStruct((half_k, cols), jnp.bfloat16),
            jax.ShapeDtypeStruct((3, rows, 2 * half_k), jnp.bfloat16),
        ),
        in_specs=[hbm] * 2,
        out_specs=(pl.BlockSpec(memory_space=pltpu.VMEM),) + (hbm,) * 2,
        scratch_shapes=[
            pltpu.VMEM((SLICES, 4 * chunk, kt), jnp.bfloat16),
            pltpu.VMEM((SLOTS, kt, nt), jnp.bfloat16),
            pltpu.VMEM((BUFS, 4 * chunk, cols), jnp.float32),
            pltpu.VMEM((RING, 2, chunk, cols), jnp.float32),
            pltpu.VMEM((RING, chunk, cols), jnp.float32),
            sem((B_PIECES,)), sem((B_PIECES,)),
            sem((steps, SLICES, 3)), sem((steps, SLICES, 3)),
            sem((steps, 2)), sem((steps, 2)), sem((steps, 2)), sem((steps, 2)),
            sem((2, 7)), sem((SLOTS,)), *[pltpu.SemaphoreType.REGULAR] * 4,
        ],
        compiler_params=pltpu.CompilerParams(
            collective_id=0, has_side_effects=True, vmem_limit_bytes=56 << 20),
    )(a_rows, b_rows)
    return outs[0]


def solution(mesh):
    spec = P(("mp", "dp"), None)

    def local(a_rows, b_rows):
        return _product(a_rows, b_rows, min(64, a_rows.shape[0] // 4))

    return jax.shard_map(local, mesh=mesh, in_specs=(spec, spec), out_specs=spec, check_vma=False)
```
